16 devices in a mesh: dp: 2 (over y, z), tp: 8 (over x, core).
Axes of the slice: x: 4, y: 2, z: 1, core: 2. Of those that a mesh axis runs over, the one named last changes fastest.
The devices are a block of a 4x4x8 slice.
Arguments:
- x_in: bfloat16 [512, 4096], P('dp'), parts along dimension 0
- w_q: bfloat16 [2, 4096, 4096], P(None, None, 'tp')
- w_k: bfloat16 [2, 4096, 1024], P(None, None, 'tp')
- w_v: bfloat16 [2, 4096, 1024], P(None, None, 'tp')
- w_o: bfloat16 [2, 4096, 4096], P(None, 'tp')
- w_gate: bfloat16 [2, 4096, 14336], P(None, None, 'tp')
- w_up: bfloat16 [2, 4096, 14336], P(None, None, 'tp')
- w_down: bfloat16 [2, 14336, 4096], P(None, 'tp')
- norm_gain: bfloat16 [2, 4096], replicated
- k_cache: bfloat16 [2, 512, 8, 64, 128], P(None, 'dp', 'tp'), parts along dimension 1
- v_cache: bfloat16 [2, 512, 8, 64, 128], P(None, 'dp', 'tp'), parts along dimension 1
- lengths: int32 [512], P('dp'), parts along dimension 0
Outputs:
- output 1: bfloat16 [512, 4096], P('dp'), parts along dimension 0
- output 2: bfloat16 [2, 512, 8, 128], P(None, 'dp', 'tp'), parts along dimension 1
- output 3: bfloat16 [2, 512, 8, 128], P(None, 'dp', 'tp'), parts along dimension 1
There are 2 independent parts. The reference program is written for one: setup_inputs(seed, part) draws one part's arguments, and reference() takes and returns one part's arrays. A program takes and returns all parts, laid end to end along the dimension named above; an argument that names none is the same for every part.
All inputs are finite; a program needn't handle non-finite values.
Results may differ from the reference program's by a relative error of at most 0.0169927.
Values are sent between devices in bfloat16 or wider.
A program may use at most 768 MiB of HBM per device.

```python
import math
import jax
import jax.numpy as jnp
from jax import lax

D = 4096
HEADS = 32
KV_HEADS = 8
HEAD = 128
FF = 14336
LAYERS = 2
BATCH = 256
CACHE_LEN = 64
ROPE_BASE = 10000
NORM_EPS = 1e-5


def draw_lengths(rng_key):
    sub_keys = jax.random.split(rng_key, 3)
    short_len = CACHE_LEN // 8
    drawn_len = jax.random.randint(sub_keys[0], (BATCH,), short_len, CACHE_LEN + 1, dtype=jnp.int32)
    first_row = jax.random.randint(sub_keys[1], (), 0, BATCH, dtype=jnp.int32)
    second_row = (first_row + 1 + jax.random.randint(sub_keys[2], (), 0, BATCH - 1, dtype=jnp.int32)) % BATCH
    row_ids = jnp.arange(BATCH, dtype=jnp.int32)
    drawn_len = jnp.where(row_ids == first_row, CACHE_LEN, drawn_len)
    return jnp.where(row_ids == second_row, short_len, drawn_len)


def normal_bf16(rng_key, arr_shape, std_scale):
    return (jax.random.normal(rng_key, arr_shape, jnp.float32) * std_scale).astype(jnp.bfloat16)


def setup_inputs(seed: int = 0, part: int = 0) -> dict:
    root_key = jax.random.key(seed)
    shared = jax.random.split(root_key, 8)
    own_keys = jax.random.split(jax.random.fold_in(root_key, part), 5)
    q_width = HEADS * HEAD
    kv_width = KV_HEADS * HEAD
    key_scale = math.sqrt(2.0 * math.log(CACHE_LEN) / 3.0)
    cache_shape = (LAYERS, BATCH, KV_HEADS, CACHE_LEN, HEAD)
    v_mean = jax.random.normal(own_keys[3], (LAYERS, BATCH, KV_HEADS, 1, HEAD), jnp.float32)
    v_noise = jax.random.normal(own_keys[4], cache_shape, jnp.float32)
    return {
        'x_in': normal_bf16(own_keys[0], (BATCH, D), 1.0),
        'w_q': normal_bf16(shared[0], (LAYERS, D, q_width), D ** -0.5),
        'w_k': normal_bf16(shared[1], (LAYERS, D, kv_width), key_scale * D ** -0.5),
        'w_v': normal_bf16(shared[2], (LAYERS, D, kv_width), D ** -0.5),
        'w_o': normal_bf16(shared[3], (LAYERS, q_width, D), q_width ** -0.5),
        'w_gate': normal_bf16(shared[4], (LAYERS, D, FF), D ** -0.5),
        'w_up': normal_bf16(shared[5], (LAYERS, D, FF), D ** -0.5),
        'w_down': normal_bf16(shared[6], (LAYERS, FF, D), 1.5 * FF ** -0.5),
        'norm_gain': jax.random.uniform(shared[7], (LAYERS, D), jnp.float32, 0.5, 1.5).astype(jnp.bfloat16),
        'k_cache': normal_bf16(own_keys[1], cache_shape, key_scale),
        'v_cache': (v_mean + v_noise).astype(jnp.bfloat16),
        'lengths': draw_lengths(own_keys[2]),
    }


def rms_norm(x_rows, gain_row):
    x_f32 = x_rows.astype(jnp.float32)
    mean_sq = jnp.mean(x_f32 * x_f32, axis=-1, keepdims=True)
    return (x_f32 * lax.rsqrt(mean_sq + NORM_EPS) * gain_row.astype(jnp.float32)).astype(jnp.bfloat16)


def rotate(values, positions):
    half_dim = values.shape[-1] // 2
    inv_freq = ROPE_BASE ** (-jnp.arange(half_dim, dtype=jnp.float32) / half_dim)
    angles = positions.astype(jnp.float32)[:, None, None] * inv_freq
    cos_ang = jnp.cos(angles)
    sin_ang = jnp.sin(angles)
    lo_half = values[..., :half_dim]
    hi_half = values[..., half_dim:]
    return jnp.concatenate([lo_half * cos_ang - hi_half * sin_ang, hi_half * cos_ang + lo_half * sin_ang], axis=-1)


def attend(q_rot, k_rot, v_val, k_layer, v_layer, lengths):
    score_scale = 1.0 / math.sqrt(q_rot.shape[-1])
    q_f32 = q_rot.astype(jnp.float32)
    scores = jnp.einsum('bkgd,bktd->bkgt', q_f32, k_layer.astype(jnp.float32)) * score_scale
    positions = jnp.arange(k_layer.shape[2], dtype=jnp.int32)
    valid_mask = positions[None, :] < lengths[:, None]
    scores = jnp.where(valid_mask[:, None, None, :], scores, -jnp.inf)
    new_score = jnp.einsum('bkgd,bkd->bkg', q_f32, k_rot.astype(jnp.float32)) * score_scale
    top_score = jnp.maximum(jnp.max(scores, axis=-1), new_score)
    cache_wts = jnp.exp(scores - top_score[..., None])
    new_wts = jnp.exp(new_score - top_score)
    denom_sum = jnp.sum(cache_wts, axis=-1) + new_wts
    cache_part = jnp.einsum('bkgt,bktd->bkgd', cache_wts.astype(jnp.bfloat16).astype(jnp.float32), v_layer.astype(jnp.float32))
    new_part = new_wts.astype(jnp.bfloat16).astype(jnp.float32)[..., None] * v_val.astype(jnp.float32)[:, :, None, :]
    return ((cache_part + new_part) / denom_sum[..., None]).astype(jnp.bfloat16)


def reference(x_in, w_q, w_k, w_v, w_o, w_gate, w_up, w_down, norm_gain, k_cache, v_cache, lengths):
    batch_rows = x_in.shape[0]
    group_size = HEADS // KV_HEADS

    def layer_step(x_cur, params):
        wq_layer, wk_layer, wv_layer, wo_layer, wg_layer, wu_layer, wd_layer, gain_layer, k_layer, v_layer = params
        normed = rms_norm(x_cur, gain_layer)
        q_f32 = jnp.dot(normed, wq_layer, preferred_element_type=jnp.float32).reshape(batch_rows, HEADS, HEAD)
        q_rot = rotate(q_f32, lengths).astype(jnp.bfloat16).reshape(batch_rows, KV_HEADS, group_size, HEAD)
        k_f32 = jnp.dot(normed, wk_layer, preferred_element_type=jnp.float32).reshape(batch_rows, KV_HEADS, HEAD)
        k_rot = rotate(k_f32, lengths).astype(jnp.bfloat16)
        v_val = jnp.dot(normed, wv_layer, preferred_element_type=jnp.float32).astype(jnp.bfloat16).reshape(batch_rows, KV_HEADS, HEAD)
        attn_heads = attend(q_rot, k_rot, v_val, k_layer, v_layer, lengths)
        attn_out = jnp.dot(attn_heads.reshape(batch_rows, HEADS * HEAD), wo_layer, preferred_element_type=jnp.float32)
        gate_val = jnp.dot(normed, wg_layer, preferred_element_type=jnp.float32)
        up_val = jnp.dot(normed, wu_layer, preferred_element_type=jnp.float32)
        act_val = (jax.nn.silu(gate_val) * up_val).astype(jnp.bfloat16)
        mlp_out = jnp.dot(act_val, wd_layer, preferred_element_type=jnp.float32)
        x_next = (x_cur.astype(jnp.float32) + (attn_out + mlp_out)).astype(jnp.bfloat16)
        return x_next, (k_rot, v_val)

    x_out, new_pairs = lax.scan(layer_step, x_in, (w_q, w_k, w_v, w_o, w_gate, w_up, w_down, norm_gain, k_cache, v_cache))
    return x_out, new_pairs[0], new_pairs[1]
```

```python
import functools
import math

import jax
import jax.numpy as jnp
import numpy as np
from jax import lax
from jax.experimental import pallas as pl
from jax.experimental.pallas import tpu as pltpu
from jax.sharding import PartitionSpec as P

ROPE_BASE = 10000
NORM_EPS = 1e-5
MESH = pl.DeviceIdType.MESH
F32 = jnp.float32
BF16 = jnp.bfloat16

ROW_GROUP = 8
KV_PIECES = 4
GROUPS = 4


def kernel(dims, x_hbm, wq, wk, wv, wo, wg, wu, wd, gain, kc, vc, lens, freq,
           xo, kn, vn,
           xb, acc, hb, wa, wb, kb, vb, lhs, qs, ks, vs, ob, lenb, cosb, sinb, rowscale, gains, kst, vst,
           send_d, recv_d, send_o, send_r, send_l, opp_t, opp_b, from_l, from_r, own, hold_r, hold_l, stat_s, stat_r,
           sem_a, sem_kv, sem_b, sem_x, sem_kn,
           d_send, d_recv, o_send, o_recv, r_send, l_send, fl_recv, fr_recv,
           ag_send, ag_fwd, ag_ring, ag_recv, st_send, st_recv):
    layers, rows, width, q_width, head, ff, cache_len, members = dims
    heads = q_width // head
    blk = width // members
    chunk = blk // 2
    half = rows // 2
    n_in = q_width + 2 * head + 2 * ff
    k_out = q_width + ff
    chips = members // 2

    me = lax.axis_index("tp")
    core = me % 2
    chip = me // 2
    mate = 2 * chip + 1 - core
    right_chip = (chip + 1) % chips
    left_chip = (chip + 3) % chips
    opp_chip = (chip + 2) % chips
    right = 2 * right_chip + core
    left = 2 * left_chip + core

    def dev(i):
        return {"tp": i}

    def chunk_id(g, q):
        turn = (g + (g // 2) * (2 * g - 3)) % 4
        if q % 2:
            turn = (4 - turn) % 4
        c = core if q < 2 else 1 - core
        return 2 * (2 * ((chip + turn) % chips) + c) + q % 2

    cols = ((wq, 0, q_width), (wk, q_width, head), (wv, q_width + head, head),
            (wg, q_width + 2 * head, ff), (wu, q_width + 2 * head + ff, ff))

    def a_copies(l, g, slot):
        out = []
        for q in range(4):
            row = pl.multiple_of(chunk_id(g, q) * chunk, chunk)
            for n, (w, at, size) in enumerate(cols):
                out.append(pltpu.make_async_copy(
                    w.at[l, pl.ds(row, chunk), :],
                    wa.at[slot, pl.ds(q * chunk, chunk), pl.ds(at, size)],
                    sem_a.at[slot, q, n]))
        return out

    piece = rows // KV_PIECES

    def kv_copies(l, p):
        at = pl.multiple_of(p * piece, piece)
        return [pltpu.make_async_copy(src.at[l, pl.ds(at, piece), 0], dst.at[pl.ds(at, piece)], sem_kv.at[n, p])
                for n, (src, dst) in enumerate(((kc, kb), (vc, vb)))]

    def b_copies(l):
        out = [pltpu.make_async_copy(wo.at[l], wb.at[pl.ds(0, q_width)], sem_b.at[0])]
        part = ff // 4
        for n in range(4):
            out.append(pltpu.make_async_copy(
                wd.at[l, pl.ds(n * part, part), :], wb.at[pl.ds(q_width + n * part, part)], sem_b.at[1 + n]))
        return out

    def x_copy(n):
        return pltpu.make_async_copy(x_hbm.at[:, pl.ds(n * chunk, chunk)], xb.at[n], sem_x.at[n])

    def out_copy(n):
        at = pl.multiple_of(n * chunk, chunk)
        return pltpu.make_async_copy(xb.at[n], xo.at[:, pl.ds(at, chunk)], sem_x.at[n])

    def kn_copies(l):
        return [pltpu.make_async_copy(kst, kn.at[l], sem_kn.at[0]), pltpu.make_async_copy(vst, vn.at[l], sem_kn.at[1])]

    def start(copies):
        for c in copies:
            c.start()

    def wait(copies):
        for c in copies:
            c.wait()

    def remote(src, dst, s, r, to):
        return pltpu.make_async_remote_copy(src_ref=src, dst_ref=dst, send_sem=s, recv_sem=r,
                                            device_id=dev(to), device_id_type=MESH)

    def mate_copy(n):
        return remote(send_d.at[n], recv_d.at[n], d_send.at[n], d_recv.at[n], mate)

    top, bottom = pl.ds(0, half), pl.ds(half, half)
    opp_right = remote(send_o.at[top], opp_t, o_send.at[0], o_recv.at[0], right)
    opp_left = remote(send_o.at[bottom], opp_b, o_send.at[1], o_recv.at[1], left)
    right_top = remote(send_r.at[top], from_l.at[top], r_send.at[0], fl_recv.at[0], right)
    right_bottom = remote(send_r.at[bottom], from_l.at[bottom], r_send.at[1], fl_recv.at[1], right)
    left_top = remote(send_l.at[top], from_r.at[top], l_send.at[0], fr_recv.at[0], left)
    left_bottom = remote(send_l.at[bottom], from_r.at[bottom], l_send.at[1], fr_recv.at[1], left)

    def x_send(n, s, to):
        return remote(xb.at[n], xb.at[n], s, ag_recv.at[n], to)

    own_a, own_b = 2 * me, 2 * me + 1
    own_sends = [x_send(own_a, ag_send.at[0], left), x_send(own_b, ag_send.at[1], right),
                 x_send(own_a, ag_send.at[2], mate), x_send(own_b, ag_send.at[3], mate),
                 x_send(own_b, ag_send.at[4], left), x_send(own_a, ag_send.at[5], right)]

    def mate_forward(g, q):
        return x_send(chunk_id(g, q), ag_fwd.at[g, q], mate)

    def ring_forward(q):
        return x_send(chunk_id(1, q), ag_ring.at[q], right if q else left)

    def arrived(n):
        x_send(n, ag_send.at[0], mate).wait_recv()

    def when(cond, fn):
        if isinstance(cond, bool):
            if cond:
                fn()
        else:
            pl.when(cond)(fn)

    def gather_step(g):
        def from_links():
            for q in range(2):
                arrived(chunk_id(g, q))
                when(g == 1, lambda q=q: ring_forward(q).start())
                mate_forward(g, q).start()
        when(g > 0, from_links)
        for q in range(2, 4):
            arrived(chunk_id(g, q))

    def gather_drain():
        for c in own_sends:
            c.wait_send()
        for g in range(1, GROUPS):
            for q in range(2):
                mate_forward(g, q).wait_send()
        for q in range(2):
            ring_forward(q).wait_send()

    def stat_copy(k):
        to = (me + k) % members
        return remote(stat_s, stat_r.at[k - 1], st_send.at[k - 1], st_recv.at[k - 1], to)

    for n in range(width // chunk):
        x_copy(n).start()
    start(a_copies(0, 0, 0))
    barrier = pltpu.get_barrier_semaphore()
    for k in range(1, members):
        pl.semaphore_signal(barrier, inc=1, device_id=dev((me + k) % members), device_id_type=MESH)
    start(a_copies(0, 1, 1))

    len_f = jnp.transpose(jnp.broadcast_to(lens[...].astype(F32), (head, rows)))
    lenb[...] = len_f
    angle = len_f * freq[...]
    cosb[...] = jnp.cos(angle)
    lane = lax.broadcasted_iota(jnp.int32, (rows, head), 1)
    sin = jnp.sin(angle)
    sinb[...] = jnp.where(lane < head // 2, -sin, sin)
    g32 = gain[...].astype(F32)
    for l in range(layers):
        gains[l] = g32[l:l + 1]

    total = jnp.zeros((rows, chunk), F32)
    for n in range(width // chunk):
        x_copy(n).wait()
    for n in range(width // chunk):
        v = xb[n].astype(F32)
        total = total + v * v
    mean = jnp.sum(total, axis=1, keepdims=True) / width
    rowscale[...] = jnp.broadcast_to(lax.rsqrt(mean + NORM_EPS), (rows, head))
    pl.semaphore_wait(barrier, members - 1)

    scale = 1.0 / math.sqrt(head)

    def layer(l, _):
        def norm_from_stats():
            s = stat_s[...]
            for k in range(1, members):
                stat_copy(k).wait_recv()
            for k in range(1, members):
                s = s + stat_r[k - 1]
            r = lax.rsqrt(s[0:1] / width + NORM_EPS)
            rowscale[...] = jnp.transpose(jnp.broadcast_to(r, (head, rows)))
        when(l > 0, norm_from_stats)

        def group(g, _):
            slot = g % 2
            when(l > 0, lambda: gather_step(g))
            r = rowscale[...]
            r = jnp.concatenate([r] * (chunk // head), axis=1)
            for q in range(4):
                n = chunk_id(g, q)
                gv = gains[l, :, pl.ds(pl.multiple_of(n * chunk, chunk), chunk)]
                hb[:, q * chunk:(q + 1) * chunk] = (xb[n].astype(F32) * r * gv).astype(BF16)
            wait(a_copies(l, g, slot))
            for at in range(0, n_in, 512):
                end = min(at + 512, n_in)
                d = jnp.dot(hb[...], wa[slot, :, at:end], preferred_element_type=F32)
                acc[:, at:end] = jnp.where(g == 0, d, acc[:, at:end] + d)
            when(g < GROUPS - 2, lambda: start(a_copies(l, g + 2, slot)))

            def later():
                for p in range(KV_PIECES):
                    start(kv_copies(l, p))
                start(b_copies(l))
            if layers > 1:
                pl.when(jnp.logical_and(l == 0, g == GROUPS - 2))(later)
            return 0
        lax.fori_loop(0, GROUPS, group, 0)

        cosv, sinv = cosb[...], sinb[...]
        for h in range(heads):
            v = acc[:, h * head:(h + 1) * head]
            qs[h] = (v * cosv + pltpu.roll(v, head // 2, 1) * sinv).astype(BF16).astype(F32)
        v = acc[:, q_width:q_width + head]
        kr = (v * cosv + pltpu.roll(v, head // 2, 1) * sinv).astype(BF16)
        vr = acc[:, q_width + head:q_width + 2 * head].astype(BF16)
        ks[...] = kr.astype(F32)
        vs[...] = vr.astype(F32)
        kst[...] = kr
        vst[...] = vr
        start(kn_copies(l))

        gate_at = q_width + 2 * head
        for at in range(0, ff, 256):
            gv = acc[:, gate_at + at:gate_at + at + 256]
            uv = acc[:, gate_at + ff + at:gate_at + ff + at + 256]
            lhs[:, q_width + at:q_width + at + 256] = (gv * jax.nn.sigmoid(gv) * uv).astype(BF16)

        tiles = ROW_GROUP * cache_len // head
        per_tile = head // cache_len
        r_id = lax.broadcasted_iota(jnp.int32, (1, ROW_GROUP, head), 1)
        lane3 = lax.broadcasted_iota(jnp.int32, (1, ROW_GROUP, head), 2)
        tile_of = r_id // per_tile
        in_row = (lane3 // cache_len) == (r_id % per_tile)
        slot_pos = (lane3 % cache_len).astype(F32)

        def attend(at):
            at = pl.multiple_of(at, ROW_GROUP)
            q3 = qs[:, pl.ds(at, ROW_GROUP), :]
            k_new = ks[pl.ds(at, ROW_GROUP), :][None]
            v_new = vs[pl.ds(at, ROW_GROUP), :][None]
            ln = lenb[pl.ds(at, ROW_GROUP), :][None]
            keys = kb[pl.ds(at, ROW_GROUP)].reshape(ROW_GROUP * cache_len, head)
            vals = vb[pl.ds(at, ROW_GROUP)].reshape(ROW_GROUP * cache_len, head)
            q2 = q3.reshape(heads * ROW_GROUP, head).astype(BF16)
            s = lax.dot_general(q2, keys, (((1,), (1,)), ((), ())), preferred_element_type=F32)
            pick = s[:, 0:head].reshape(heads, ROW_GROUP, head)
            for j in range(1, tiles):
                pick = jnp.where(tile_of == j, s[:, j * head:(j + 1) * head].reshape(heads, ROW_GROUP, head), pick)
            ok = jnp.logical_and(in_row, slot_pos < ln)
            sc = jnp.where(ok, pick * scale, -jnp.inf)
            s_new = jnp.sum(q3 * k_new, axis=-1, keepdims=True) * scale
            peak = jnp.maximum(jnp.max(sc, axis=-1, keepdims=True), s_new)
            w = jnp.exp(sc - peak)
            w_new = jnp.exp(s_new - peak)
            den = jnp.sum(w, axis=-1, keepdims=True) + w_new
            parts = [jnp.where(tile_of == j, w, 0.0).reshape(heads * ROW_GROUP, head).astype(BF16) for j in range(tiles)]
            pv = jnp.dot(jnp.concatenate(parts, axis=1), vals, preferred_element_type=F32)
            o = (pv.reshape(heads, ROW_GROUP, head) + w_new.astype(BF16).astype(F32) * v_new) / den
            for h in range(heads):
                ob[pl.ds(at, ROW_GROUP), h * head:(h + 1) * head] = o[h]

        def attend_piece(p, _):
            wait(kv_copies(l, p))

            def step(i, _):
                for u in range(2):
                    attend(p * piece + i * (2 * ROW_GROUP) + u * ROW_GROUP)
                return 0
            lax.fori_loop(0, piece // (2 * ROW_GROUP), step, 0)
            return 0
        lax.fori_loop(0, KV_PIECES, attend_piece, 0)
        lhs[:, 0:q_width] = ob[...].astype(BF16)

        def prefetch():
            start(a_copies(l + 1, 0, 0))
            for p in range(KV_PIECES):
                start(kv_copies(l + 1, p))
            start(a_copies(l + 1, 1, 1))
        when(l < layers - 1, prefetch)
        wait(kn_copies(l))
        when(l > 0, gather_drain)

        wait(b_copies(l))

        def share(i):
            at = pl.multiple_of(i * blk, blk)
            return jnp.dot(lhs[...], wb[:, pl.ds(at, blk)], preferred_element_type=F32)

        send_d[0] = share(2 * opp_chip + 1 - core).astype(BF16)
        mate_copy(0).start()
        send_d[1] = share(2 * right_chip + 1 - core).astype(BF16)
        mate_copy(1).start()
        t = share(2 * opp_chip + core)
        mate_copy(0).wait_recv()
        send_o[...] = (t + recv_d[0].astype(F32)).astype(BF16)
        opp_right.start()
        opp_left.start()
        send_d[2] = share(2 * left_chip + 1 - core).astype(BF16)
        mate_copy(2).start()
        t = share(right)
        mate_copy(1).wait_recv()
        t = t + recv_d[1].astype(F32)
        send_r[bottom] = t[half:].astype(BF16)
        right_bottom.start()
        hold_r[...] = t[:half]
        t = share(left)
        mate_copy(2).wait_recv()
        t = t + recv_d[2].astype(F32)
        send_l[top] = t[:half].astype(BF16)
        left_top.start()
        hold_l[...] = t[half:]
        send_d[3] = share(mate).astype(BF16)
        mate_copy(3).start()
        own[...] = share(me)
        when(l < layers - 1, lambda: start(b_copies(l + 1)))
        opp_right.wait_recv()
        send_r[top] = (hold_r[...] + opp_t[...].astype(F32)).astype(BF16)
        right_top.start()
        opp_left.wait_recv()
        send_l[bottom] = (hold_l[...] + opp_b[...].astype(F32)).astype(BF16)
        left_bottom.start()
        mate_copy(3).wait_recv()
        x_old = jnp.concatenate([xb[own_a], xb[own_b]], axis=1).astype(F32)
        own[...] = own[...] + recv_d[3].astype(F32) + x_old
        right_bottom.wait_recv()
        left_top.wait_recv()
        right_top.wait_recv()
        left_bottom.wait_recv()
        x_new = (own[...] + from_l[...].astype(F32) + from_r[...].astype(F32)).astype(BF16)
        xb[own_a] = x_new[:, :chunk]
        xb[own_b] = x_new[:, chunk:]

        def send_stats():
            v = x_new.astype(F32)
            v = v * v
            part = v[:, 0:head]
            for at in range(head, blk, head):
                part = part + v[:, at:at + head]
            col = jnp.broadcast_to(jnp.sum(part, axis=1, keepdims=True), (rows, head))
            stat_s[...] = jnp.transpose(col)[0:8]
            for k in range(1, members):
                stat_copy(k).start()
        when(l < layers - 1, send_stats)
        for c in own_sends:
            c.start()
        for n in range(4):
            mate_copy(n).wait_send()
        for c in (opp_right, opp_left, right_top, right_bottom, left_top, left_bottom):
            c.wait_send()

        def drain_stats():
            for k in range(1, members):
                stat_copy(k).wait_send()
        when(l < layers - 1, drain_stats)
        return 0

    lax.fori_loop(0, layers, layer, 0)

    out_copy(own_a).start()
    out_copy(own_b).start()
    for g in range(1, GROUPS):
        for q in range(2):
            arrived(chunk_id(g, q))
            if g == 1:
                ring_forward(q).start()
            mate_forward(g, q).start()
            out_copy(chunk_id(g, q)).start()
    for g in range(GROUPS):
        for q in range(2, 4):
            arrived(chunk_id(g, q))
            out_copy(chunk_id(g, q)).start()
    gather_drain()
    for n in range(width // chunk):
        out_copy(n).wait()


def solution(mesh):
    members = mesh.shape["tp"]
    weight_col = P(None, None, "tp")
    weight_row = P(None, "tp", None)
    cache_spec = P(None, "dp", "tp", None, None)
    new_spec = P(None, "dp", "tp", None)
    row_spec = P("dp", None)
    arg_specs = (row_spec, weight_col, weight_col, weight_col, weight_row, weight_col, weight_col, weight_row,
                 P(None, None), cache_spec, cache_spec, P("dp"))

    def per_device(x_in, w_q, w_k, w_v, w_o, w_gate, w_up, w_down, norm_gain, k_cache, v_cache, lengths):
        rows, width = x_in.shape
        layers, _, q_width = w_q.shape
        cache_len, head = k_cache.shape[-2:]
        ff = w_gate.shape[-1]
        dims = (layers, rows, width, q_width, head, ff, cache_len, members)
        blk = width // members
        chunk = blk // 2
        half = rows // 2
        n_in = q_width + 2 * head + 2 * ff
        inv = np.float32(ROPE_BASE) ** (-np.arange(head // 2, dtype=np.float32) / np.float32(head // 2))
        freq = jnp.asarray(np.concatenate([inv, inv])[None].astype(np.float32))
        vmem = pl.BlockSpec(memory_space=pltpu.VMEM)
        hbm = pl.BlockSpec(memory_space=pl.ANY)
        dma = pltpu.SemaphoreType.DMA
        x_out, k_new, v_new = pl.pallas_call(
            functools.partial(kernel, dims),
            out_shape=(jax.ShapeDtypeStruct((rows, width), BF16),
                       jax.ShapeDtypeStruct((layers, rows, head), BF16),
                       jax.ShapeDtypeStruct((layers, rows, head), BF16)),
            in_specs=[hbm] * 8 + [vmem, hbm, hbm, vmem, vmem],
            out_specs=(hbm, hbm, hbm),
            scratch_shapes=[
                pltpu.VMEM((width // chunk, rows, chunk), BF16),
                pltpu.VMEM((rows, n_in), F32),
                pltpu.VMEM((rows, 4 * chunk), BF16),
                pltpu.VMEM((2, 4 * chunk, n_in), BF16),
                pltpu.VMEM((q_width + ff, width), BF16),
                pltpu.VMEM((rows, cache_len, head), BF16),
                pltpu.VMEM((rows, cache_len, head), BF16),
                pltpu.VMEM((rows, q_width + ff), BF16),
                pltpu.VMEM((q_width // head, rows, head), F32),
                pltpu.VMEM((rows, head), F32),
                pltpu.VMEM((rows, head), F32),
                pltpu.VMEM((rows, q_width), F32),
                pltpu.VMEM((rows, head), F32),
                pltpu.VMEM((rows, head), F32),
                pltpu.VMEM((rows, head), F32),
                pltpu.VMEM((rows, head), F32),
                pltpu.VMEM((layers, 1, width), F32),
                pltpu.VMEM((rows, head), BF16),
                pltpu.VMEM((rows, head), BF16),
                pltpu.VMEM((4, rows, blk), BF16),
                pltpu.VMEM((4, rows, blk), BF16),
                pltpu.VMEM((rows, blk), BF16),
                pltpu.VMEM((rows, blk), BF16),
                pltpu.VMEM((rows, blk), BF16),
                pltpu.VMEM((half, blk), BF16),
                pltpu.VMEM((half, blk), BF16),
                pltpu.VMEM((rows, blk), BF16),
                pltpu.VMEM((rows, blk), BF16),
                pltpu.VMEM((rows, blk), F32),
                pltpu.VMEM((half, blk), F32),
                pltpu.VMEM((half, blk), F32),
                pltpu.VMEM((8, rows), F32),
                pltpu.VMEM((members - 1, 8, rows), F32),
                dma((2, 4, 5)), dma((2, KV_PIECES)), dma((5,)), dma((width // chunk,)), dma((2,)),
                dma((4,)), dma((4,)), dma((2,)), dma((2,)), dma((2,)), dma((2,)), dma((2,)), dma((2,)),
                dma((6,)), dma((GROUPS, 2)), dma((2,)), dma((width // chunk,)),
                dma((members - 1,)), dma((members - 1,)),
            ],
            compiler_params=pltpu.CompilerParams(
                collective_id=0, has_side_effects=True, vmem_limit_bytes=67043328),
        )(x_in, w_q, w_k, w_v, w_o, w_gate, w_up, w_down, norm_gain, k_cache, v_cache,
          lengths.reshape(1, rows), freq)
        return x_out, k_new.reshape(layers, rows, 1, head), v_new.reshape(layers, rows, 1, head)

    return jax.shard_map(per_device, mesh=mesh, in_specs=arg_specs, out_specs=(row_spec, new_spec, new_spec),
                         check_vma=False)
```

```python
import functools
import math

import jax
import jax.numpy as jnp
import numpy as np
from jax import lax
from jax.experimental import pallas as pl
from jax.experimental.pallas import tpu as pltpu
from jax.sharding import PartitionSpec as P

ROPE_BASE = 10000
NORM_EPS = 1e-5
MESH = pl.DeviceIdType.MESH
F32 = jnp.float32
BF16 = jnp.bfloat16

ROW_GROUP = 8
STEP_ROWS = 32
KV_PIECES = 4
PLACE_PIECES = 8
GROUPS = 4


def kernel(dims, x_hbm, wq, wk, wv, wo, wg, wu, wd, gain, kc, vc, lens, freq,
           xo, kn, vn,
           xb, acc, hb, wa, wb, kb, vb, lhs, qs, ks, vs, ob, lenb, cosb, sinb, rowscale, gains, kst, vst,
           send_d, recv_d, send_o, send_r, send_l, opp_t, opp_b, from_l, from_r, own, hold_r, hold_l, stat_s, stat_r,
           sem_a, sem_kv, sem_b, sem_x, sem_kn,
           d_send, d_recv, o_send, o_recv, r_send, l_send, fl_recv, fr_recv,
           ag_send, ag_fwd, ag_ring, ag_recv, st_send, st_recv):
    layers, rows, width, q_width, head, ff, cache_len, members = dims
    heads = q_width // head
    blk = width // members
    chunk = blk // 2
    half = rows // 2
    n_in = q_width + 2 * head + 2 * ff
    k_out = q_width + ff
    chips = members // 2

    me = lax.axis_index("tp")
    core = me % 2
    chip = me // 2
    mate = 2 * chip + 1 - core
    right_chip = (chip + 1) % chips
    left_chip = (chip + 3) % chips
    opp_chip = (chip + 2) % chips
    right = 2 * right_chip + core
    left = 2 * left_chip + core

    def dev(i):
        return {"tp": i}

    def chunk_id(g, q):
        turn = (g + (g // 2) * (2 * g - 3)) % 4
        if q % 2:
            turn = (4 - turn) % 4
        c = core if q < 2 else 1 - core
        return 2 * (2 * ((chip + turn) % chips) + c) + q % 2

    cols = ((wq, 0, q_width), (wk, q_width, head), (wv, q_width + head, head),
            (wg, q_width + 2 * head, ff), (wu, q_width + 2 * head + ff, ff))

    def a_copies(l, g, slot, which=range(5)):
        out = []
        for q in range(4):
            row = pl.multiple_of(chunk_id(g, q) * chunk, chunk)
            for n in which:
                w, at, size = cols[n]
                out.append(pltpu.make_async_copy(
                    w.at[l, pl.ds(row, chunk), :],
                    wa.at[slot, pl.ds(q * chunk, chunk), pl.ds(at, size)],
                    sem_a.at[slot, q, n]))
        return out

    piece = rows // KV_PIECES

    def start_kv(l):
        for p in range(KV_PIECES):
            start(kv_copies(l, p))

    def kv_copies(l, p):
        at = pl.multiple_of(p * piece, piece)
        return [pltpu.make_async_copy(src.at[l, pl.ds(at, piece), 0], dst.at[pl.ds(at, piece)], sem_kv.at[n, p])
                for n, (src, dst) in enumerate(((kc, kb), (vc, vb)))]

    def b_copies(l):
        out = [pltpu.make_async_copy(wo.at[l], wb.at[pl.ds(0, q_width)], sem_b.at[0])]
        part = ff // 4
        for n in range(4):
            out.append(pltpu.make_async_copy(
                wd.at[l, pl.ds(n * part, part), :], wb.at[pl.ds(q_width + n * part, part)], sem_b.at[1 + n]))
        return out

    def x_copy(n):
        return pltpu.make_async_copy(x_hbm.at[:, pl.ds(n * chunk, chunk)], xb.at[n], sem_x.at[n])

    def out_copy(n):
        at = pl.multiple_of(n * chunk, chunk)
        return pltpu.make_async_copy(xb.at[n], xo.at[:, pl.ds(at, chunk)], sem_x.at[n])

    def kn_copies(l):
        return [pltpu.make_async_copy(kst, kn.at[l], sem_kn.at[0]), pltpu.make_async_copy(vst, vn.at[l], sem_kn.at[1])]

    def start(copies):
        for c in copies:
            c.start()

    def wait(copies):
        for c in copies:
            c.wait()

    def remote(src, dst, s, r, to):
        return pltpu.make_async_remote_copy(src_ref=src, dst_ref=dst, send_sem=s, recv_sem=r,
                                            device_id=dev(to), device_id_type=MESH)

    def mate_copy(n):
        return remote(send_d.at[n], recv_d.at[n], d_send.at[n], d_recv.at[n], mate)

    top, bottom = pl.ds(0, half), pl.ds(half, half)
    opp_right = remote(send_o.at[top], opp_t, o_send.at[0], o_recv.at[0], right)
    opp_left = remote(send_o.at[bottom], opp_b, o_send.at[1], o_recv.at[1], left)
    right_top = remote(send_r.at[top], from_l.at[top], r_send.at[0], fl_recv.at[0], right)
    right_bottom = remote(send_r.at[bottom], from_l.at[bottom], r_send.at[1], fl_recv.at[1], right)
    left_top = remote(send_l.at[top], from_r.at[top], l_send.at[0], fr_recv.at[0], left)
    left_bottom = remote(send_l.at[bottom], from_r.at[bottom], l_send.at[1], fr_recv.at[1], left)

    def x_send(n, s, to):
        return remote(xb.at[n], xb.at[n], s, ag_recv.at[n], to)

    own_a, own_b = 2 * me, 2 * me + 1
    own_sends = [x_send(own_a, ag_send.at[0], left), x_send(own_b, ag_send.at[1], right),
                 x_send(own_a, ag_send.at[2], mate), x_send(own_b, ag_send.at[3], mate),
                 x_send(own_b, ag_send.at[4], left), x_send(own_a, ag_send.at[5], right)]

    def mate_forward(g, q):
        return x_send(chunk_id(g, q), ag_fwd.at[g, q], mate)

    def ring_forward(q):
        return x_send(chunk_id(1, q), ag_ring.at[q], right if q else left)

    def arrived(n):
        x_send(n, ag_send.at[0], mate).wait_recv()

    def when(cond, fn):
        if isinstance(cond, bool):
            if cond:
                fn()
        else:
            pl.when(cond)(fn)

    def gather_links(g):
        for q in range(2):
            arrived(chunk_id(g, q))
            when(g == 1, lambda q=q: ring_forward(q).start())
            mate_forward(g, q).start()

    def gather_mate(g):
        for q in range(2, 4):
            arrived(chunk_id(g, q))

    def sum_drain():
        for n in range(4):
            mate_copy(n).wait_send()
        for c in (opp_right, opp_left, right_top, right_bottom, left_top, left_bottom):
            c.wait_send()

    def gather_drain():
        for c in own_sends:
            c.wait_send()
        for g in range(1, GROUPS):
            for q in range(2):
                mate_forward(g, q).wait_send()
        for q in range(2):
            ring_forward(q).wait_send()

    def stat_copy(k):
        to = (me + k) % members
        return remote(stat_s, stat_r.at[k - 1], st_send.at[k - 1], st_recv.at[k - 1], to)

    for n in range(width // chunk):
        x_copy(n).start()
    start(a_copies(0, 0, 0))
    barrier = pltpu.get_barrier_semaphore()
    for k in range(1, members):
        pl.semaphore_signal(barrier, inc=1, device_id=dev((me + k) % members), device_id_type=MESH)
    start(a_copies(0, 1, 1))

    len_f = jnp.transpose(jnp.broadcast_to(lens[...].astype(F32), (head, rows)))
    lenb[...] = len_f
    angle = len_f * freq[...]
    cosb[...] = jnp.cos(angle)
    lane = lax.broadcasted_iota(jnp.int32, (rows, head), 1)
    sin = jnp.sin(angle)
    sinb[...] = jnp.where(lane < head // 2, -sin, sin)
    g32 = gain[...].astype(F32)
    for l in range(layers):
        gains[l] = g32[l:l + 1]

    total = jnp.zeros((rows, chunk), F32)
    for n in range(width // chunk):
        x_copy(n).wait()
        v = xb[n].astype(F32)
        total = total + v * v
    mean = jnp.sum(total, axis=1, keepdims=True) / width
    rowscale[...] = jnp.broadcast_to(lax.rsqrt(mean + NORM_EPS), (rows, head))
    pl.semaphore_wait(barrier, members - 1)

    scale = 1.0 / math.sqrt(head)

    def layer(l, _):
        def norm_from_stats():
            s = stat_s[...]
            for k in range(1, members):
                stat_copy(k).wait_recv()
            for k in range(1, members):
                s = s + stat_r[k - 1]
            r = lax.rsqrt(s[0:1] / width + NORM_EPS)
            rowscale[...] = jnp.transpose(jnp.broadcast_to(r, (head, rows)))
        when(l > 0, norm_from_stats)

        def group(g, _):
            slot = g % 2
            when(l > 0, lambda: gather_mate(g))
            r = rowscale[...]
            r = jnp.concatenate([r] * (chunk // head), axis=1)
            for q in range(4):
                n = chunk_id(g, q)
                gv = gains[l, :, pl.ds(pl.multiple_of(n * chunk, chunk), chunk)]
                hb[:, q * chunk:(q + 1) * chunk] = (xb[n].astype(F32) * r * gv).astype(BF16)
            wait(a_copies(l, g, slot))

            def product(at, end):
                d = jnp.dot(hb[...], wa[slot, :, at:end], preferred_element_type=F32)
                acc[:, at:end] = jnp.where(g == 0, d, acc[:, at:end] + d)

            cuts = list(range(0, n_in, 512)) + [n_in]
            gate_end = q_width + 2 * head + ff
            middle = next(n for n, at in enumerate(cuts) if at >= gate_end)
            for at, end in zip(cuts[:middle], cuts[1:middle + 1]):
                product(at, end)
            when(g < GROUPS - 2, lambda: start(a_copies(l, g + 2, slot, range(4))))
            pl.when(jnp.logical_and(l > 0, g < GROUPS - 1))(lambda: gather_links(g + 1))
            pl.when(jnp.logical_and(l == 0, g == GROUPS - 2))(lambda: start_kv(l))
            for at, end in zip(cuts[middle:-1], cuts[middle + 1:]):
                product(at, end)
            when(g < GROUPS - 2, lambda: start(a_copies(l, g + 2, slot, range(4, 5))))
            pl.when(jnp.logical_and(l == 0, g == GROUPS - 2))(lambda: start(b_copies(l)))
            return 0
        lax.fori_loop(0, GROUPS, group, 0)

        cosv, sinv = cosb[...], sinb[...]
        for h in range(heads):
            v = acc[:, h * head:(h + 1) * head]
            qs[h] = (v * cosv + pltpu.roll(v, head // 2, 1) * sinv).astype(BF16).astype(F32)
        v = acc[:, q_width:q_width + head]
        kr = (v * cosv + pltpu.roll(v, head // 2, 1) * sinv).astype(BF16)
        vr = acc[:, q_width + head:q_width + 2 * head].astype(BF16)
        ks[...] = kr.astype(F32)
        vs[...] = vr.astype(F32)
        kst[...] = kr
        vst[...] = vr
        start(kn_copies(l))

        gate_at = q_width + 2 * head
        for at in range(0, ff, 256):
            gv = acc[:, gate_at + at:gate_at + at + 256]
            uv = acc[:, gate_at + ff + at:gate_at + ff + at + 256]
            lhs[:, q_width + at:q_width + at + 256] = (gv * jax.nn.sigmoid(gv) * uv).astype(BF16)

        tiles = ROW_GROUP * cache_len // head
        per_tile = head // cache_len
        r_id = lax.broadcasted_iota(jnp.int32, (1, ROW_GROUP, head), 1)
        lane3 = lax.broadcasted_iota(jnp.int32, (1, ROW_GROUP, head), 2)
        tile_of = r_id // per_tile
        in_row = (lane3 // cache_len) == (r_id % per_tile)
        slot_pos = (lane3 % cache_len).astype(F32)

        def scores(at):
            keys = kb[at:at + ROW_GROUP].reshape(ROW_GROUP * cache_len, head)
            q2 = qs[:, at:at + ROW_GROUP, :].reshape(heads * ROW_GROUP, head).astype(BF16)
            s = lax.dot_general(q2, keys, (((1,), (1,)), ((), ())), preferred_element_type=F32)
            pick = s[:, 0:head].reshape(heads, ROW_GROUP, head)
            for j in range(1, tiles):
                pick = jnp.where(tile_of == j, s[:, j * head:(j + 1) * head].reshape(heads, ROW_GROUP, head), pick)
            return pick

        def weights(at, pick):
            ok = jnp.logical_and(in_row, slot_pos < lenb[at:at + ROW_GROUP, :][None])
            sc = jnp.where(ok, pick * scale, -jnp.inf)
            s_new = jnp.sum(qs[:, at:at + ROW_GROUP, :] * ks[at:at + ROW_GROUP, :][None], axis=-1, keepdims=True) * scale
            peak = jnp.maximum(jnp.max(sc, axis=-1, keepdims=True), s_new)
            w = jnp.exp(sc - peak)
            w_new = jnp.exp(s_new - peak)
            return w, w_new, jnp.sum(w, axis=-1, keepdims=True) + w_new

        def mix(at, w, w_new, den):
            vals = vb[at:at + ROW_GROUP].reshape(ROW_GROUP * cache_len, head)
            parts = [jnp.where(tile_of == j, w, 0.0).reshape(heads * ROW_GROUP, head).astype(BF16) for j in range(tiles)]
            pv = jnp.dot(jnp.concatenate(parts, axis=1), vals, preferred_element_type=F32)
            o = (pv.reshape(heads, ROW_GROUP, head) + w_new.astype(BF16).astype(F32) * vs[at:at + ROW_GROUP, :][None]) / den
            for h in range(heads):
                ob[at:at + ROW_GROUP, h * head:(h + 1) * head] = o[h]

        for p in range(KV_PIECES):
            wait(kv_copies(l, p))
        step = STEP_ROWS
        groups_at = [list(range(b, b + step, ROW_GROUP)) for b in range(0, rows, step)]
        picks, wts = {}, {}
        for b in range(len(groups_at) + 2):
            if b < len(groups_at):
                for at in groups_at[b]:
                    picks[at] = scores(at)
            if 0 <= b - 2:
                for at in groups_at[b - 2]:
                    mix(at, *wts.pop(at))
            if 0 <= b - 1 < len(groups_at):
                for at in groups_at[b - 1]:
                    wts[at] = weights(at, picks.pop(at))
        lhs[:, 0:q_width] = ob[...].astype(BF16)

        def prefetch():
            start(a_copies(l + 1, 0, 0))
            start_kv(l + 1)
            start(a_copies(l + 1, 1, 1))
        when(l < layers - 1, prefetch)
        wait(kn_copies(l))

        def drain():
            sum_drain()
            gather_drain()
            for k in range(1, members):
                stat_copy(k).wait_send()
        when(l > 0, drain)

        wait(b_copies(l))

        def share(i):
            at = pl.multiple_of(i * blk, blk)
            return jnp.dot(lhs[...], wb[:, pl.ds(at, blk)], preferred_element_type=F32)

        send_d[0] = share(2 * opp_chip + 1 - core).astype(BF16)
        mate_copy(0).start()
        own[...] = share(2 * opp_chip + core)
        send_d[1] = share(2 * right_chip + 1 - core).astype(BF16)
        mate_copy(1).start()
        mate_copy(0).wait_recv()
        send_o[...] = (own[...] + recv_d[0].astype(F32)).astype(BF16)
        opp_right.start()
        opp_left.start()
        send_d[2] = share(2 * left_chip + 1 - core).astype(BF16)
        mate_copy(2).start()
        t = share(right)
        mate_copy(1).wait_recv()
        t = t + recv_d[1].astype(F32)
        send_r[bottom] = t[half:].astype(BF16)
        right_bottom.start()
        hold_r[...] = t[:half]
        t = share(left)
        mate_copy(2).wait_recv()
        t = t + recv_d[2].astype(F32)
        send_l[top] = t[:half].astype(BF16)
        left_top.start()
        hold_l[...] = t[half:]
        send_d[3] = share(mate).astype(BF16)
        mate_copy(3).start()
        own[...] = share(me)
        when(l < layers - 1, lambda: start(b_copies(l + 1)))
        opp_right.wait_recv()
        send_r[top] = (hold_r[...] + opp_t[...].astype(F32)).astype(BF16)
        right_top.start()
        opp_left.wait_recv()
        send_l[bottom] = (hold_l[...] + opp_b[...].astype(F32)).astype(BF16)
        left_bottom.start()
        mate_copy(3).wait_recv()
        x_old = jnp.concatenate([xb[own_a], xb[own_b]], axis=1).astype(F32)
        own[...] = own[...] + recv_d[3].astype(F32) + x_old
        right_bottom.wait_recv()
        left_top.wait_recv()
        right_top.wait_recv()
        left_bottom.wait_recv()
        x_new = (own[...] + from_l[...].astype(F32) + from_r[...].astype(F32)).astype(BF16)
        xb[own_a] = x_new[:, :chunk]
        xb[own_b] = x_new[:, chunk:]

        def send_stats():
            v = x_new.astype(F32)
            v = v * v
            part = v[:, 0:head]
            for at in range(head, blk, head):
                part = part + v[:, at:at + head]
            col = jnp.broadcast_to(jnp.sum(part, axis=1, keepdims=True), (rows, head))
            stat_s[...] = jnp.transpose(col)[0:8]
            for k in range(1, members):
                stat_copy(k).start()
        when(l < layers - 1, send_stats)
        for c in own_sends:
            c.start()
        return 0

    lax.fori_loop(0, layers, layer, 0)

    out_copy(own_a).start()
    out_copy(own_b).start()
    for g in range(1, GROUPS):
        gather_links(g)
        for q in range(2):
            out_copy(chunk_id(g, q)).start()
    for g in range(GROUPS):
        gather_mate(g)
        for q in range(2, 4):
            out_copy(chunk_id(g, q)).start()
    sum_drain()
    gather_drain()
    for n in range(width // chunk):
        out_copy(n).wait()


def place(x, kn, vn, xo, ko, vo, xt, kt, vt, sem_in, sem_out):
    part = x.shape[0] // PLACE_PIECES
    loads, stores = [], []
    for n in range(PLACE_PIECES):
        r = pl.ds(n * part, part)
        loads.append(pltpu.make_async_copy(x.at[r], xt.at[r], sem_in.at[n]))
        stores.append(pltpu.make_async_copy(xt.at[r], xo.at[r], sem_out.at[n]))
    for n, (src, mid, dst) in enumerate(((kn, kt, ko), (vn, vt, vo))):
        loads.append(pltpu.make_async_copy(src, mid, sem_in.at[PLACE_PIECES + n]))
        stores.append(pltpu.make_async_copy(mid, dst, sem_out.at[PLACE_PIECES + n]))
    for c in loads:
        c.start()
    for a, b in zip(loads, stores):
        a.wait()
        b.start()
    for c in stores:
        c.wait()


def solution(mesh):
    members = mesh.shape["tp"]
    weight_col = P(None, None, "tp")
    weight_row = P(None, "tp", None)
    cache_spec = P(None, "dp", "tp", None, None)
    new_spec = P(None, "dp", "tp", None)
    row_spec = P("dp", None)
    arg_specs = (row_spec, weight_col, weight_col, weight_col, weight_row, weight_col, weight_col, weight_row,
                 P(None, None), cache_spec, cache_spec, P("dp"))

    def per_device(x_in, w_q, w_k, w_v, w_o, w_gate, w_up, w_down, norm_gain, k_cache, v_cache, lengths):
        rows, width = x_in.shape
        layers, _, q_width = w_q.shape
        cache_len, head = k_cache.shape[-2:]
        ff = w_gate.shape[-1]
        dims = (layers, rows, width, q_width, head, ff, cache_len, members)
        blk = width // members
        chunk = blk // 2
        half = rows // 2
        n_in = q_width + 2 * head + 2 * ff
        inv = np.float32(ROPE_BASE) ** (-np.arange(head // 2, dtype=np.float32) / np.float32(head // 2))
        freq = jnp.asarray(np.concatenate([inv, inv])[None].astype(np.float32))
        vmem = pl.BlockSpec(memory_space=pltpu.VMEM)
        hbm = pl.BlockSpec(memory_space=pl.ANY)
        dma = pltpu.SemaphoreType.DMA
        x_out, k_new, v_new = pl.pallas_call(
            functools.partial(kernel, dims),
            out_shape=(jax.ShapeDtypeStruct((rows, width), BF16),
                       jax.ShapeDtypeStruct((layers, rows, head), BF16),
                       jax.ShapeDtypeStruct((layers, rows, head), BF16)),
            in_specs=[hbm] * 8 + [vmem, hbm, hbm, vmem, vmem],
            out_specs=(hbm, hbm, hbm),
            scratch_shapes=[
                pltpu.VMEM((width // chunk, rows, chunk), BF16),
                pltpu.VMEM((rows, n_in), F32),
                pltpu.VMEM((rows, 4 * chunk), BF16),
                pltpu.VMEM((2, 4 * chunk, n_in), BF16),
                pltpu.VMEM((q_width + ff, width), BF16),
                pltpu.VMEM((rows, cache_len, head), BF16),
                pltpu.VMEM((rows, cache_len, head), BF16),
                pltpu.VMEM((rows, q_width + ff), BF16),
                pltpu.VMEM((q_width // head, rows, head), F32),
                pltpu.VMEM((rows, head), F32),
                pltpu.VMEM((rows, head), F32),
                pltpu.VMEM((rows, q_width), F32),
                pltpu.VMEM((rows, head), F32),
                pltpu.VMEM((rows, head), F32),
                pltpu.VMEM((rows, head), F32),
                pltpu.VMEM((rows, head), F32),
                pltpu.VMEM((layers, 1, width), F32),
                pltpu.VMEM((rows, head), BF16),
                pltpu.VMEM((rows, head), BF16),
                pltpu.VMEM((4, rows, blk), BF16),
                pltpu.VMEM((4, rows, blk), BF16),
                pltpu.VMEM((rows, blk), BF16),
                pltpu.VMEM((rows, blk), BF16),
                pltpu.VMEM((rows, blk), BF16),
                pltpu.VMEM((half, blk), BF16),
                pltpu.VMEM((half, blk), BF16),
                pltpu.VMEM((rows, blk), BF16),
                pltpu.VMEM((rows, blk), BF16),
                pltpu.VMEM((rows, blk), F32),
                pltpu.VMEM((half, blk), F32),
                pltpu.VMEM((half, blk), F32),
                pltpu.VMEM((8, rows), F32),
                pltpu.VMEM((members - 1, 8, rows), F32),
                dma((2, 4, 5)), dma((2, KV_PIECES)), dma((5,)), dma((width // chunk,)), dma((2,)),
                dma((4,)), dma((4,)), dma((2,)), dma((2,)), dma((2,)), dma((2,)), dma((2,)), dma((2,)),
                dma((6,)), dma((GROUPS, 2)), dma((2,)), dma((width // chunk,)),
                dma((members - 1,)), dma((members - 1,)),
            ],
            compiler_params=pltpu.CompilerParams(
                collective_id=0, has_side_effects=True, vmem_limit_bytes=67043328),
        )(x_in, w_q, w_k, w_v, w_o, w_gate, w_up, w_down, norm_gain, k_cache, v_cache,
          lengths.reshape(1, rows), freq)
        results = (x_out, k_new, v_new)
        x_out, k_new, v_new = pl.pallas_call(
            place,
            out_shape=tuple(jax.ShapeDtypeStruct(a.shape, a.dtype) for a in results),
            in_specs=[hbm] * 3,
            out_specs=(hbm,) * 3,
            scratch_shapes=[pltpu.VMEM(a.shape, a.dtype) for a in results]
            + [dma((PLACE_PIECES + 2,)), dma((PLACE_PIECES + 2,))],
        )(*results)
        return x_out, k_new.reshape(layers, rows, 1, head), v_new.reshape(layers, rows, 1, head)

    return jax.shard_map(per_device, mesh=mesh, in_specs=arg_specs, out_specs=(row_spec, new_spec, new_spec),
                         check_vma=False)
```

```python
import functools
import math

import jax
import jax.numpy as jnp
import numpy as np
from jax import lax
from jax.experimental import pallas as pl
from jax.experimental.pallas import tpu as pltpu
from jax.sharding import PartitionSpec as P

ROPE_BASE = 10000
NORM_EPS = 1e-5
MESH = pl.DeviceIdType.MESH
F32 = jnp.float32
BF16 = jnp.bfloat16

ROW_GROUP = 8
STEP_ROWS = 32
KV_PIECES = 4
PLACE_PIECES = 8
GROUPS = 4


def kernel(dims, x_hbm, wq, wk, wv, wo, wg, wu, wd, gain_hbm, kc, vc, lens_hbm, freq_hbm,
           xo, kn, vn,
           xb, acc, hb, wa, wb, kb, vb, lhs, qs, ks, vs, ob, lenb, cosb, sinb, rowscale, gains, kst, vst,
           gain, lens, freq, send_d, recv_d, send_o, send_r, send_l, opp_t, opp_b, from_l, from_r, own, hold_r, hold_l, stat_s, stat_r,
           sem_a, sem_kv, sem_b, sem_x, sem_kn, sem_s,
           d_send, d_recv, o_send, o_recv, r_send, l_send, fl_recv, fr_recv,
           ag_send, ag_fwd, ag_ring, ag_recv, st_send, st_recv):
    layers, rows, width, q_width, head, ff, cache_len, members = dims
    heads = q_width // head
    blk = width // members
    chunk = blk // 2
    half = rows // 2
    n_in = q_width + 2 * head + 2 * ff
    k_out = q_width + ff
    chips = members // 2

    me = lax.axis_index("tp")
    core = me % 2
    chip = me // 2
    mate = 2 * chip + 1 - core
    right_chip = (chip + 1) % chips
    left_chip = (chip + 3) % chips
    opp_chip = (chip + 2) % chips
    right = 2 * right_chip + core
    left = 2 * left_chip + core

    def dev(i):
        return {"tp": i}

    def chunk_id(g, q):
        turn = (g + (g // 2) * (2 * g - 3)) % 4
        if q % 2:
            turn = (4 - turn) % 4
        c = (core + q // 2) % 2
        return 2 * (2 * ((chip + turn) % chips) + c) + q % 2

    def step_chunk(i, ab):
        g = i // 2
        turn = (g + (g // 2) * (2 * g - 3)) % 4
        if ab:
            turn = (4 - turn) % 4
        return 2 * (2 * ((chip + turn) % chips) + (core + i) % 2) + ab

    def step_copies(l, i, which=range(2)):
        out = []
        for ab in which:
            row = pl.multiple_of(step_chunk(i, ab) * chunk, chunk)
            at = pl.multiple_of((i % 2) * 2 * chunk, chunk) + ab * chunk
            for n, (w, to, size) in enumerate(cols):
                out.append(pltpu.make_async_copy(
                    w.at[l, pl.ds(row, chunk), :],
                    wa.at[(i // 2) % 2, pl.ds(at, chunk), pl.ds(to, size)],
                    sem_a.at[(i // 2) % 2, (i % 2) * 2 + ab, n]))
        return out

    cols = ((wq, 0, q_width), (wk, q_width, head), (wv, q_width + head, head),
            (wg, q_width + 2 * head, ff), (wu, q_width + 2 * head + ff, ff))

    def a_copies(l, g, slot, which=range(5), parts=range(4)):
        out = []
        for q in parts:
            row = pl.multiple_of(chunk_id(g, q) * chunk, chunk)
            for n in which:
                w, at, size = cols[n]
                out.append(pltpu.make_async_copy(
                    w.at[l, pl.ds(row, chunk), :],
                    wa.at[slot, pl.ds(q * chunk, chunk), pl.ds(at, size)],
                    sem_a.at[slot, q, n]))
        return out

    piece = rows // KV_PIECES

    def start_kv(l, n):
        for p in range(KV_PIECES):
            kv_copy(l, p, n).start()

    def kv_copy(l, p, n):
        src, dst = ((kc, kb), (vc, vb))[n]
        at = pl.ds(p * piece, piece)
        return pltpu.make_async_copy(src.at[l, at, 0], dst.at[at], sem_kv.at[n, p])

    def start_kv(l, n):
        for p in range(KV_PIECES):
            kv_copy(l, p, n).start()

    def kv_copies(l, p):
        at = pl.multiple_of(p * piece, piece)
        return [pltpu.make_async_copy(src.at[l, pl.ds(at, piece), 0], dst.at[pl.ds(at, piece)], sem_kv.at[n, p])
                for n, (src, dst) in enumerate(((kc, kb), (vc, vb)))]

    b_order = (opp_chip, right_chip, left_chip, chip)

    def b_copies(l, n):
        at = pl.ds(pl.multiple_of(b_order[n] * 2 * blk, 2 * blk), 2 * blk)
        return [pltpu.make_async_copy(wo.at[l, :, at], wb.at[pl.ds(0, q_width), at], sem_b.at[n, 0]),
                pltpu.make_async_copy(wd.at[l, :, at], wb.at[pl.ds(q_width, ff), at], sem_b.at[n, 1])]

    def start_b(l):
        for n in range(4):
            start(b_copies(l, n))

    def x_copy(n):
        return pltpu.make_async_copy(x_hbm.at[:, pl.ds(n * chunk, chunk)], xb.at[n], sem_x.at[n])

    def out_copy(n):
        at = pl.multiple_of(n * chunk, chunk)
        return pltpu.make_async_copy(xb.at[n], xo.at[:, pl.ds(at, chunk)], sem_x.at[n])

    def kn_copies(l):
        return [pltpu.make_async_copy(kst, kn.at[l], sem_kn.at[0]), pltpu.make_async_copy(vst, vn.at[l], sem_kn.at[1])]

    def start(copies):
        for c in copies:
            c.start()

    def wait(copies):
        for c in copies:
            c.wait()

    def remote(src, dst, s, r, to):
        return pltpu.make_async_remote_copy(src_ref=src, dst_ref=dst, send_sem=s, recv_sem=r,
                                            device_id=dev(to), device_id_type=MESH)

    def mate_copy(n):
        return remote(send_d.at[n], recv_d.at[n], d_send.at[n], d_recv.at[n], mate)

    top, bottom = pl.ds(0, half), pl.ds(half, half)
    mate_top = remote(send_d.at[0, top], recv_d.at[0, top], d_send.at[0], d_recv.at[0], mate)
    mate_bottom = remote(send_d.at[0, bottom], recv_d.at[0, bottom], d_send.at[4], d_recv.at[4], mate)
    opp_right = remote(send_o.at[top], opp_t, o_send.at[0], o_recv.at[0], right)
    opp_left = remote(send_o.at[bottom], opp_b, o_send.at[1], o_recv.at[1], left)
    right_top = remote(send_r.at[top], from_l.at[top], r_send.at[0], fl_recv.at[0], right)
    right_bottom = remote(send_r.at[bottom], from_l.at[bottom], r_send.at[1], fl_recv.at[1], right)
    left_top = remote(send_l.at[top], from_r.at[top], l_send.at[0], fr_recv.at[0], left)
    left_bottom = remote(send_l.at[bottom], from_r.at[bottom], l_send.at[1], fr_recv.at[1], left)

    def x_send(n, s, to):
        return remote(xb.at[n], xb.at[n], s, ag_recv.at[n], to)

    own_a, own_b = 2 * me, 2 * me + 1
    own_sends = [x_send(own_a, ag_send.at[0], left), x_send(own_b, ag_send.at[1], right),
                 x_send(own_a, ag_send.at[2], mate), x_send(own_b, ag_send.at[3], mate),
                 x_send(own_b, ag_send.at[4], left), x_send(own_a, ag_send.at[5], right)]

    def mate_forward(g, q):
        return x_send(chunk_id(g, q), ag_fwd.at[g, q], mate)

    def ring_forward(q):
        return x_send(chunk_id(1, q), ag_ring.at[q], right if q else left)

    def arrived(n):
        x_send(n, ag_send.at[0], mate).wait_recv()

    def when(cond, fn):
        if isinstance(cond, bool):
            if cond:
                fn()
        else:
            pl.when(cond)(fn)

    def gather_links(g):
        for q in range(2):
            arrived(chunk_id(g, q))
            when(g == 1, lambda q=q: ring_forward(q).start())
            mate_forward(g, q).start()

    def gather_mate(g):
        for q in range(2, 4):
            arrived(chunk_id(g, q))

    def sum_drain():
        for n in range(1, 4):
            mate_copy(n).wait_send()
        for c in (mate_top, mate_bottom, opp_right, opp_left, right_top, right_bottom, left_top, left_bottom):
            c.wait_send()

    def gather_drain():
        for c in own_sends:
            c.wait_send()
        for g in range(1, GROUPS):
            for q in range(2):
                mate_forward(g, q).wait_send()
        for q in range(2):
            ring_forward(q).wait_send()

    def stat_copy(k):
        to = (me + k) % members
        return remote(stat_s, stat_r.at[k - 1], st_send.at[k - 1], st_recv.at[k - 1], to)

    small = [pltpu.make_async_copy(a, b, sem_s.at[n])
             for n, (a, b) in enumerate(((lens_hbm, lens), (freq_hbm, freq), (gain_hbm, gain)))]
    start(small)
    for n in range(width // chunk):
        x_copy(n).start()
    start(step_copies(0, 0, (0,)))
    barrier = pltpu.get_barrier_semaphore()
    for k in range(1, members):
        pl.semaphore_signal(barrier, inc=1, device_id=dev((me + k) % members), device_id_type=MESH)
    wait(small)
    start(step_copies(0, 0, (1,)))
    len_f = jnp.transpose(jnp.broadcast_to(lens[...].astype(F32), (head, rows)))
    lenb[...] = len_f
    angle = len_f * freq[...]
    cosb[...] = jnp.cos(angle)
    lane = lax.broadcasted_iota(jnp.int32, (rows, head), 1)
    sin = jnp.sin(angle)
    sinb[...] = jnp.where(lane < head // 2, -sin, sin)
    for n in range(width // chunk):
        x_copy(n).wait()
    start(step_copies(0, 1))
    g32 = gain[...].astype(F32)
    for l in range(layers):
        gains[l] = g32[l:l + 1]
    total = jnp.zeros((rows, chunk), F32)
    for n in range(width // chunk):
        v = xb[n].astype(F32)
        total = total + v * v
    mean = jnp.sum(total, axis=1, keepdims=True) / width
    rowscale[...] = jnp.broadcast_to(lax.rsqrt(mean + NORM_EPS), (rows, head))

    scale = 1.0 / math.sqrt(head)

    def layer(l):
        def norm_from_stats():
            s = stat_s[...]
            for k in range(1, members):
                stat_copy(k).wait_recv()
            for k in range(1, members):
                s = s + stat_r[k - 1]
            r = lax.rsqrt(s[0:1] / width + NORM_EPS)
            rowscale[...] = jnp.transpose(jnp.broadcast_to(r, (head, rows)))
        when(l > 0, norm_from_stats)

        def normed_chunk(n):
            r = rowscale[...]
            r = jnp.concatenate([r] * (chunk // head), axis=1)
            gv = gains[l, :, pl.ds(pl.multiple_of(n * chunk, chunk), chunk)]
            return (xb[n].astype(F32) * r * gv).astype(BF16)

        def normed(g, qs):
            for q in qs:
                hb[:, (4 * g + q) * chunk:(4 * g + q + 1) * chunk] = normed_chunk(chunk_id(g, q))

        cuts = list(range(0, n_in, 512)) + [n_in]
        gate_end = q_width + 2 * head + ff
        middle = next(n for n, at in enumerate(cuts) if at >= gate_end)

        def products(g, spans):
            for at, end in spans:
                d = jnp.dot(hb[:, 4 * g * chunk:4 * (g + 1) * chunk], wa[g % 2, :, at:end], preferred_element_type=F32)
                acc[:, at:end] = d if g == 0 else acc[:, at:end] + d

        spans = list(zip(cuts[:-1], cuts[1:]))

        def stream_step(i, first):
            wait(step_copies(l, i))
            k_at = pl.ds(pl.multiple_of(i * 2 * chunk, 2 * chunk), 2 * chunk)
            rows_at = pl.ds(pl.multiple_of((i % 2) * 2 * chunk, chunk), 2 * chunk)
            for at, end in spans:
                d = jnp.dot(hb[:, k_at], wa[(i // 2) % 2, rows_at, at:end], preferred_element_type=F32)
                acc[:, at:end] = d if first else acc[:, at:end] + d

        if l == 0:
            for g in range(GROUPS):
                normed(g, range(4))
            start(step_copies(l, 2))
            start(step_copies(l, 3))
            stream_step(0, True)
            start(step_copies(l, 4))

            def stream(i, _):
                stream_step(i, False)
                start(step_copies(l, i + 4))
                return 0
            lax.fori_loop(1, 4, stream, 0)

            def group(g, _):
                slot = g % 2
                wait(a_copies(l, g, slot))
                k_at = pl.ds(pl.multiple_of(g * 4 * chunk, 4 * chunk), 4 * chunk)
                for at, end in spans:
                    acc[:, at:end] += jnp.dot(hb[:, k_at], wa[slot, :, at:end], preferred_element_type=F32)

                def after_two():
                    start_kv(l, 0)
                    start_kv(l, 1)
                pl.when(g == 2)(after_two)

                def after_three():
                    start(b_copies(l, 0))
                    start(b_copies(l, 1))
                pl.when(g == 3)(after_three)
                return 0
            lax.fori_loop(2, GROUPS, group, 0)
        else:
            for g in range(GROUPS):
                slot = g % 2
                gather_mate(g)
                normed(g, range(4) if g == 0 else range(2, 4))
                wait(a_copies(l, g, slot))
                products(g, spans[:middle])
                if g < GROUPS - 2:
                    start(a_copies(l, g + 2, slot, range(4)))
                if g < GROUPS - 1:
                    gather_links(g + 1)
                    normed(g + 1, range(2))
                products(g, spans[middle:])
                if g < GROUPS - 2:
                    start(a_copies(l, g + 2, slot, range(4, 5)))

        cosv, sinv = cosb[...], sinb[...]
        for h in range(heads):
            v = acc[:, h * head:(h + 1) * head]
            qs[h] = (v * cosv + pltpu.roll(v, head // 2, 1) * sinv).astype(BF16).astype(F32)
        v = acc[:, q_width:q_width + head]
        kr = (v * cosv + pltpu.roll(v, head // 2, 1) * sinv).astype(BF16)
        vr = acc[:, q_width + head:q_width + 2 * head].astype(BF16)
        ks[...] = kr.astype(F32)
        vs[...] = vr.astype(F32)
        kst[...] = kr
        vst[...] = vr
        start(kn_copies(l))

        gate_at = q_width + 2 * head
        for at in range(0, ff, 256):
            gv = acc[:, gate_at + at:gate_at + at + 256]
            uv = acc[:, gate_at + ff + at:gate_at + ff + at + 256]
            lhs[:, q_width + at:q_width + at + 256] = (gv * jax.nn.sigmoid(gv) * uv).astype(BF16)

        if l == 0:
            start(b_copies(l, 2))
            start(b_copies(l, 3))
        tiles = ROW_GROUP * cache_len // head
        per_tile = head // cache_len
        r_id = lax.broadcasted_iota(jnp.int32, (1, ROW_GROUP, head), 1)
        lane3 = lax.broadcasted_iota(jnp.int32, (1, ROW_GROUP, head), 2)
        tile_of = r_id // per_tile
        in_row = (lane3 // cache_len) == (r_id % per_tile)
        slot_pos = (lane3 % cache_len).astype(F32)

        def scores(at):
            keys = kb[at:at + ROW_GROUP].reshape(ROW_GROUP * cache_len, head)
            q2 = qs[:, at:at + ROW_GROUP, :].reshape(heads * ROW_GROUP, head).astype(BF16)
            s = lax.dot_general(q2, keys, (((1,), (1,)), ((), ())), preferred_element_type=F32)
            pick = s[:, 0:head].reshape(heads, ROW_GROUP, head)
            for j in range(1, tiles):
                pick = jnp.where(tile_of == j, s[:, j * head:(j + 1) * head].reshape(heads, ROW_GROUP, head), pick)
            return pick

        def weights(at, pick):
            ok = jnp.logical_and(in_row, slot_pos < lenb[at:at + ROW_GROUP, :][None])
            sc = jnp.where(ok, pick * scale, -jnp.inf)
            s_new = jnp.sum(qs[:, at:at + ROW_GROUP, :] * ks[at:at + ROW_GROUP, :][None], axis=-1, keepdims=True) * scale
            peak = jnp.maximum(jnp.max(sc, axis=-1, keepdims=True), s_new)
            w = jnp.exp(sc - peak)
            w_new = jnp.exp(s_new - peak)
            return w, w_new, jnp.sum(w, axis=-1, keepdims=True) + w_new

        def mix(at, w, w_new, den):
            vals = vb[at:at + ROW_GROUP].reshape(ROW_GROUP * cache_len, head)
            parts = [jnp.where(tile_of == j, w, 0.0).reshape(heads * ROW_GROUP, head).astype(BF16) for j in range(tiles)]
            pv = jnp.dot(jnp.concatenate(parts, axis=1), vals, preferred_element_type=F32)
            o = (pv.reshape(heads, ROW_GROUP, head) + w_new.astype(BF16).astype(F32) * vs[at:at + ROW_GROUP, :][None]) / den
            for h in range(heads):
                ob[at:at + ROW_GROUP, h * head:(h + 1) * head] = o[h]

        for p in range(KV_PIECES):
            wait(kv_copy(l, p, n) for n in range(2))
        step = STEP_ROWS
        groups_at = [list(range(b, b + step, ROW_GROUP)) for b in range(0, rows, step)]
        picks, wts = {}, {}
        for b in range(len(groups_at) + 2):
            if b < len(groups_at):
                for at in groups_at[b]:
                    picks[at] = scores(at)
            if 0 <= b - 2:
                for at in groups_at[b - 2]:
                    mix(at, *wts.pop(at))
            if 0 <= b - 1 < len(groups_at):
                for at in groups_at[b - 1]:
                    wts[at] = weights(at, picks.pop(at))
        lhs[:, 0:q_width] = ob[...].astype(BF16)

        wait(kn_copies(l))

        def drain():
            sum_drain()
            gather_drain()
            for k in range(1, members):
                stat_copy(k).wait_send()
        when(l > 0, drain)

        wait(b_copies(l, 0))
        if l == 0:
            pl.semaphore_wait(barrier, members - 1)

        def share(i):
            at = pl.multiple_of(i * blk, blk)
            return jnp.dot(lhs[...], wb[:, pl.ds(at, blk)], preferred_element_type=F32)

        send_d[0] = share(2 * opp_chip + 1 - core).astype(BF16)
        mate_top.start()
        mate_bottom.start()
        own[...] = share(2 * opp_chip + core)
        mate_top.wait_recv()
        send_o[top] = (own[top] + recv_d[0, top].astype(F32)).astype(BF16)
        opp_right.start()
        mate_bottom.wait_recv()
        send_o[bottom] = (own[bottom] + recv_d[0, bottom].astype(F32)).astype(BF16)
        opp_left.start()
        wait(b_copies(l, 1))
        wait(b_copies(l, 2))
        send_d[1] = share(2 * right_chip + 1 - core).astype(BF16)
        send_d[2] = share(2 * left_chip + 1 - core).astype(BF16)
        mate_copy(1).start()
        mate_copy(2).start()
        hold_r[...] = share(right)
        hold_l[...] = share(left)
        mate_copy(1).wait_recv()
        send_r[bottom] = (hold_r[bottom] + recv_d[1, bottom].astype(F32)).astype(BF16)
        right_bottom.start()
        mate_copy(2).wait_recv()
        send_l[top] = (hold_l[top] + recv_d[2, top].astype(F32)).astype(BF16)
        left_top.start()
        wait(b_copies(l, 3))
        if l < layers - 1:
            start(a_copies(l + 1, 0, 0))
            start(a_copies(l + 1, 1, 1))
            start_kv(l + 1, 0)
            start_kv(l + 1, 1)
        send_d[3] = share(mate).astype(BF16)
        own[...] = share(me)
        mate_copy(3).start()
        when(l < layers - 1, lambda: start_b(l + 1))
        opp_right.wait_recv()
        send_r[top] = (hold_r[top] + recv_d[1, top].astype(F32) + opp_t[...].astype(F32)).astype(BF16)
        right_top.start()
        opp_left.wait_recv()
        send_l[bottom] = (hold_l[bottom] + recv_d[2, bottom].astype(F32) + opp_b[...].astype(F32)).astype(BF16)
        left_bottom.start()
        mate_copy(3).wait_recv()
        x_old = jnp.concatenate([xb[own_a], xb[own_b]], axis=1).astype(F32)
        own[...] = own[...] + recv_d[3].astype(F32) + x_old
        right_bottom.wait_recv()
        left_top.wait_recv()
        right_top.wait_recv()
        left_bottom.wait_recv()
        x_new = (own[...] + from_l[...].astype(F32) + from_r[...].astype(F32)).astype(BF16)
        xb[own_a] = x_new[:, :chunk]
        xb[own_b] = x_new[:, chunk:]

        def send_stats():
            v = x_new.astype(F32)
            v = v * v
            part = v[:, 0:head]
            for at in range(head, blk, head):
                part = part + v[:, at:at + head]
            col = jnp.broadcast_to(jnp.sum(part, axis=1, keepdims=True), (rows, head))
            stat_s[...] = jnp.transpose(col)[0:8]
            for k in range(1, members):
                stat_copy(k).start()
        when(l < layers - 1, send_stats)
        for c in own_sends:
            c.start()

    for l in range(layers):
        layer(l)

    out_copy(own_a).start()
    out_copy(own_b).start()
    for g in range(1, GROUPS):
        gather_links(g)
        for q in range(2):
            out_copy(chunk_id(g, q)).start()
    for g in range(GROUPS):
        gather_mate(g)
        for q in range(2, 4):
            out_copy(chunk_id(g, q)).start()
    sum_drain()
    gather_drain()
    for n in range(width // chunk):
        out_copy(n).wait()


def place(x, kn, vn, xo, ko, vo, xt, kt, vt, sem_in, sem_out):
    part = x.shape[0] // PLACE_PIECES
    loads, stores = [], []
    for n in range(PLACE_PIECES):
        r = pl.ds(n * part, part)
        loads.append(pltpu.make_async_copy(x.at[r], xt.at[r], sem_in.at[n]))
        stores.append(pltpu.make_async_copy(xt.at[r], xo.at[r], sem_out.at[n]))
    for n, (src, mid, dst) in enumerate(((kn, kt, ko), (vn, vt, vo))):
        loads.append(pltpu.make_async_copy(src, mid, sem_in.at[PLACE_PIECES + n]))
        stores.append(pltpu.make_async_copy(mid, dst, sem_out.at[PLACE_PIECES + n]))
    for c in loads:
        c.start()
    for a, b in zip(loads, stores):
        a.wait()
        b.start()
    for c in stores:
        c.wait()


def solution(mesh):
    members = mesh.shape["tp"]
    weight_col = P(None, None, "tp")
    weight_row = P(None, "tp", None)
    cache_spec = P(None, "dp", "tp", None, None)
    new_spec = P(None, "dp", "tp", None)
    row_spec = P("dp", None)
    arg_specs = (row_spec, weight_col, weight_col, weight_col, weight_row, weight_col, weight_col, weight_row,
                 P(None, None), cache_spec, cache_spec, P("dp"))

    def per_device(x_in, w_q, w_k, w_v, w_o, w_gate, w_up, w_down, norm_gain, k_cache, v_cache, lengths):
        rows, width = x_in.shape
        layers, _, q_width = w_q.shape
        cache_len, head = k_cache.shape[-2:]
        ff = w_gate.shape[-1]
        dims = (layers, rows, width, q_width, head, ff, cache_len, members)
        blk = width // members
        chunk = blk // 2
        half = rows // 2
        n_in = q_width + 2 * head + 2 * ff
        inv = np.float32(ROPE_BASE) ** (-np.arange(head // 2, dtype=np.float32) / np.float32(head // 2))
        freq = jnp.asarray(np.concatenate([inv, inv])[None].astype(np.float32))
        hbm = pl.BlockSpec(memory_space=pl.ANY)
        dma = pltpu.SemaphoreType.DMA
        x_out, k_new, v_new = pl.pallas_call(
            functools.partial(kernel, dims),
            out_shape=(jax.ShapeDtypeStruct((rows, width), BF16),
                       jax.ShapeDtypeStruct((layers, rows, head), BF16),
                       jax.ShapeDtypeStruct((layers, rows, head), BF16)),
            in_specs=[hbm] * 13,
            out_specs=(hbm, hbm, hbm),
            scratch_shapes=[
                pltpu.VMEM((width // chunk, rows, chunk), BF16),
                pltpu.VMEM((rows, n_in), F32),
                pltpu.VMEM((rows, width), BF16),
                pltpu.VMEM((2, 4 * chunk, n_in), BF16),
                pltpu.VMEM((q_width + ff, width), BF16),
                pltpu.VMEM((rows, cache_len, head), BF16),
                pltpu.VMEM((rows, cache_len, head), BF16),
                pltpu.VMEM((rows, q_width + ff), BF16),
                pltpu.VMEM((q_width // head, rows, head), F32),
                pltpu.VMEM((rows, head), F32),
                pltpu.VMEM((rows, head), F32),
                pltpu.VMEM((rows, q_width), F32),
                pltpu.VMEM((rows, head), F32),
                pltpu.VMEM((rows, head), F32),
                pltpu.VMEM((rows, head), F32),
                pltpu.VMEM((rows, head), F32),
                pltpu.VMEM((layers, 1, width), F32),
                pltpu.VMEM((rows, head), BF16),
                pltpu.VMEM((rows, head), BF16),
                pltpu.VMEM((layers, width), BF16),
                pltpu.VMEM((1, rows), jnp.int32),
                pltpu.VMEM((1, head), F32),
                pltpu.VMEM((4, rows, blk), BF16),
                pltpu.VMEM((4, rows, blk), BF16),
                pltpu.VMEM((rows, blk), BF16),
                pltpu.VMEM((rows, blk), BF16),
                pltpu.VMEM((rows, blk), BF16),
                pltpu.VMEM((half, blk), BF16),
                pltpu.VMEM((half, blk), BF16),
                pltpu.VMEM((rows, blk), BF16),
                pltpu.VMEM((rows, blk), BF16),
                pltpu.VMEM((rows, blk), F32),
                pltpu.VMEM((rows, blk), F32),
                pltpu.VMEM((rows, blk), F32),
                pltpu.VMEM((8, rows), F32),
                pltpu.VMEM((members - 1, 8, rows), F32),
                dma((2, 4, 5)), dma((2, KV_PIECES)), dma((4, 2)), dma((width // chunk,)), dma((2,)), dma((3,)),
                dma((5,)), dma((5,)), dma((2,)), dma((2,)), dma((2,)), dma((2,)), dma((2,)), dma((2,)),
                dma((6,)), dma((GROUPS, 2)), dma((2,)), dma((width // chunk,)),
                dma((members - 1,)), dma((members - 1,)),
            ],
            compiler_params=pltpu.CompilerParams(
                collective_id=0, has_side_effects=True, vmem_limit_bytes=67043328),
        )(x_in, w_q, w_k, w_v, w_o, w_gate, w_up, w_down, norm_gain, k_cache, v_cache,
          lengths.reshape(1, rows), freq)
        results = (x_out, k_new, v_new)
        x_out, k_new, v_new = pl.pallas_call(
            place,
            out_shape=tuple(jax.ShapeDtypeStruct(a.shape, a.dtype) for a in results),
            in_specs=[hbm] * 3,
            out_specs=(hbm,) * 3,
            scratch_shapes=[pltpu.VMEM(a.shape, a.dtype) for a in results]
            + [dma((PLACE_PIECES + 2,)), dma((PLACE_PIECES + 2,))],
        )(*results)
        return x_out, k_new.reshape(layers, rows, 1, head), v_new.reshape(layers, rows, 1, head)

    return jax.shard_map(per_device, mesh=mesh, in_specs=arg_specs, out_specs=(row_spec, new_spec, new_spec),
                         check_vma=False)
```

```python
import functools
import math

import jax
import jax.numpy as jnp
import numpy as np
from jax import lax
from jax.experimental import pallas as pl
from jax.experimental.pallas import tpu as pltpu
from jax.sharding import PartitionSpec as P

ROPE_BASE = 10000
NORM_EPS = 1e-5
MESH = pl.DeviceIdType.MESH
F32 = jnp.float32
BF16 = jnp.bfloat16

ROW_GROUP = 8
STEP_ROWS = 32
KV_PIECES = 4
PLACE_PIECES = 8
PHASES = ((0, 1), (2,), (3, 4), (5, 6), (7,))
GROUPS = 4


def kernel(dims, x_hbm, wq, wk, wv, wo, wg, wu, wd, gain_hbm, kc, vc, lens_hbm, freq_hbm,
           xo, kn, vn,
           xb, acc, hb, wa, wb, kb, vb, lhs, qs, ks, vs, ob, lenb, cosb, sinb, rowscale, gains, kst, vst,
           gain, lens, freq, send_d, recv_d, send_o, send_r, send_l, opp_t, opp_b, from_l, from_r, own, hold_r, hold_l, stat_s, stat_r,
           sem_a, sem_kv, sem_b, sem_x, sem_kn, sem_s,
           d_send, d_recv, o_send, o_recv, r_send, l_send, fl_recv, fr_recv,
           ag_send, ag_fwd, ag_ring, ag_recv, st_send, st_recv):
    layers, rows, width, q_width, head, ff, cache_len, members = dims
    heads = q_width // head
    blk = width // members
    chunk = blk // 2
    half = rows // 2
    n_in = q_width + 2 * head + 2 * ff
    k_out = q_width + ff
    chips = members // 2

    me = lax.axis_index("tp")
    core = me % 2
    chip = me // 2
    mate = 2 * chip + 1 - core
    right_chip = (chip + 1) % chips
    left_chip = (chip + 3) % chips
    opp_chip = (chip + 2) % chips
    right = 2 * right_chip + core
    left = 2 * left_chip + core

    def dev(i):
        return {"tp": i}

    def chunk_id(g, q):
        turn = (g + (g // 2) * (2 * g - 3)) % 4
        if q % 2:
            turn = (4 - turn) % 4
        c = (core + q // 2) % 2
        return 2 * (2 * ((chip + turn) % chips) + c) + q % 2

    def step_chunk(i, ab):
        g = i // 2
        turn = (g + (g // 2) * (2 * g - 3)) % 4
        if ab:
            turn = (4 - turn) % 4
        return 2 * (2 * ((chip + turn) % chips) + (core + i) % 2) + ab

    def step_copies(l, i, which=range(2)):
        out = []
        for ab in which:
            row = pl.multiple_of(step_chunk(i, ab) * chunk, chunk)
            at = pl.multiple_of((i % 2) * 2 * chunk, chunk) + ab * chunk
            for n, (w, to, size) in enumerate(cols):
                out.append(pltpu.make_async_copy(
                    w.at[l, pl.ds(row, chunk), :],
                    wa.at[(i // 2) % 2, pl.ds(at, chunk), pl.ds(to, size)],
                    sem_a.at[(i // 2) % 2, (i % 2) * 2 + ab, n]))
        return out

    cols = ((wq, 0, q_width), (wk, q_width, head), (wv, q_width + head, head),
            (wg, q_width + 2 * head, ff), (wu, q_width + 2 * head + ff, ff))

    def a_copies(l, g, slot, which=range(5), parts=range(4)):
        out = []
        for q in parts:
            row = pl.multiple_of(chunk_id(g, q) * chunk, chunk)
            for n in which:
                w, at, size = cols[n]
                out.append(pltpu.make_async_copy(
                    w.at[l, pl.ds(row, chunk), :],
                    wa.at[slot, pl.ds(q * chunk, chunk), pl.ds(at, size)],
                    sem_a.at[slot, q, n]))
        return out

    piece = rows // KV_PIECES

    def start_kv(l, n):
        for p in range(KV_PIECES):
            kv_copy(l, p, n).start()

    def kv_copy(l, p, n):
        src, dst = ((kc, kb), (vc, vb))[n]
        at = pl.ds(p * piece, piece)
        return pltpu.make_async_copy(src.at[l, at, 0], dst.at[at], sem_kv.at[n, p])

    def start_kv(l, n):
        for p in range(KV_PIECES):
            kv_copy(l, p, n).start()

    def kv_copies(l, p):
        at = pl.multiple_of(p * piece, piece)
        return [pltpu.make_async_copy(src.at[l, pl.ds(at, piece), 0], dst.at[pl.ds(at, piece)], sem_kv.at[n, p])
                for n, (src, dst) in enumerate(((kc, kb), (vc, vb)))]

    b_order = (opp_chip, right_chip, left_chip, chip)

    def b_copies(l, n):
        at = pl.ds(pl.multiple_of(b_order[n] * 2 * blk, 2 * blk), 2 * blk)
        return [pltpu.make_async_copy(wo.at[l, :, at], wb.at[pl.ds(0, q_width), at], sem_b.at[n, 0]),
                pltpu.make_async_copy(wd.at[l, :, at], wb.at[pl.ds(q_width, ff), at], sem_b.at[n, 1])]

    def start_b(l):
        for n in range(4):
            start(b_copies(l, n))

    def x_copy(n):
        return pltpu.make_async_copy(x_hbm.at[:, pl.ds(n * chunk, chunk)], xb.at[n], sem_x.at[n])

    def out_copy(n):
        at = pl.multiple_of(n * chunk, chunk)
        return pltpu.make_async_copy(xb.at[n], xo.at[:, pl.ds(at, chunk)], sem_x.at[n])

    def kn_copies(l):
        return [pltpu.make_async_copy(kst, kn.at[l], sem_kn.at[0]), pltpu.make_async_copy(vst, vn.at[l], sem_kn.at[1])]

    def start(copies):
        for c in copies:
            c.start()

    def wait(copies):
        for c in copies:
            c.wait()

    def remote(src, dst, s, r, to):
        return pltpu.make_async_remote_copy(src_ref=src, dst_ref=dst, send_sem=s, recv_sem=r,
                                            device_id=dev(to), device_id_type=MESH)

    def mate_copy(n):
        return remote(send_d.at[n], recv_d.at[n], d_send.at[n], d_recv.at[n], mate)

    top, bottom = pl.ds(0, half), pl.ds(half, half)
    mate_top = remote(send_d.at[0, top], recv_d.at[0, top], d_send.at[0], d_recv.at[0], mate)
    mate_bottom = remote(send_d.at[0, bottom], recv_d.at[0, bottom], d_send.at[4], d_recv.at[4], mate)
    opp_right = remote(send_o.at[top], opp_t, o_send.at[0], o_recv.at[0], right)
    opp_left = remote(send_o.at[bottom], opp_b, o_send.at[1], o_recv.at[1], left)
    right_top = remote(send_r.at[top], from_l.at[top], r_send.at[0], fl_recv.at[0], right)
    right_bottom = remote(send_r.at[bottom], from_l.at[bottom], r_send.at[1], fl_recv.at[1], right)
    left_top = remote(send_l.at[top], from_r.at[top], l_send.at[0], fr_recv.at[0], left)
    left_bottom = remote(send_l.at[bottom], from_r.at[bottom], l_send.at[1], fr_recv.at[1], left)

    def x_send(n, s, to):
        return remote(xb.at[n], xb.at[n], s, ag_recv.at[n], to)

    own_a, own_b = 2 * me, 2 * me + 1
    own_sends = [x_send(own_a, ag_send.at[0], left), x_send(own_b, ag_send.at[1], right),
                 x_send(own_a, ag_send.at[2], mate), x_send(own_b, ag_send.at[3], mate),
                 x_send(own_b, ag_send.at[4], left), x_send(own_a, ag_send.at[5], right)]

    def mate_forward(g, q):
        return x_send(chunk_id(g, q), ag_fwd.at[g, q], mate)

    def ring_forward(q):
        return x_send(chunk_id(1, q), ag_ring.at[q], right if q else left)

    def arrived(n):
        x_send(n, ag_send.at[0], mate).wait_recv()

    def when(cond, fn):
        if isinstance(cond, bool):
            if cond:
                fn()
        else:
            pl.when(cond)(fn)

    def gather_links(g):
        for q in range(2):
            arrived(chunk_id(g, q))
            when(g == 1, lambda q=q: ring_forward(q).start())
            mate_forward(g, q).start()

    def gather_mate(g):
        for q in range(2, 4):
            arrived(chunk_id(g, q))

    def sum_drain():
        for n in range(1, 4):
            mate_copy(n).wait_send()
        for c in (mate_top, mate_bottom, opp_right, opp_left, right_top, right_bottom, left_top, left_bottom):
            c.wait_send()

    def gather_drain():
        for c in own_sends:
            c.wait_send()
        for g in range(1, GROUPS):
            for q in range(2):
                mate_forward(g, q).wait_send()
        for q in range(2):
            ring_forward(q).wait_send()

    def stat_copy(k):
        to = (me + k) % members
        return remote(stat_s, stat_r.at[k - 1], st_send.at[k - 1], st_recv.at[k - 1], to)

    small = [pltpu.make_async_copy(a, b, sem_s.at[n])
             for n, (a, b) in enumerate(((lens_hbm, lens), (freq_hbm, freq), (gain_hbm, gain)))]
    start(small)
    for n in range(width // chunk):
        x_copy(n).start()
    start(step_copies(0, 0))
    barrier = pltpu.get_barrier_semaphore()
    for k in range(1, members):
        pl.semaphore_signal(barrier, inc=1, device_id=dev((me + k) % members), device_id_type=MESH)
    wait(small)
    start(step_copies(0, 1))
    len_f = jnp.transpose(jnp.broadcast_to(lens[...].astype(F32), (head, rows)))
    lenb[...] = len_f
    angle = len_f * freq[...]
    cosb[...] = jnp.cos(angle)
    lane = lax.broadcasted_iota(jnp.int32, (rows, head), 1)
    sin = jnp.sin(angle)
    sinb[...] = jnp.where(lane < head // 2, -sin, sin)
    for n in range(width // chunk):
        x_copy(n).wait()
    start(step_copies(0, 2))
    g32 = gain[...].astype(F32)
    for l in range(layers):
        gains[l] = g32[l:l + 1]
    total = jnp.zeros((rows, chunk), F32)
    for n in range(width // chunk):
        v = xb[n].astype(F32)
        total = total + v * v
    mean = jnp.sum(total, axis=1, keepdims=True) / width
    rowscale[...] = jnp.broadcast_to(lax.rsqrt(mean + NORM_EPS), (rows, head))

    scale = 1.0 / math.sqrt(head)

    def layer(l):
        def norm_from_stats():
            s = stat_s[...]
            for k in range(1, members):
                stat_copy(k).wait_recv()
            for k in range(1, members):
                s = s + stat_r[k - 1]
            r = lax.rsqrt(s[0:1] / width + NORM_EPS)
            rowscale[...] = jnp.transpose(jnp.broadcast_to(r, (head, rows)))
        when(l > 0, norm_from_stats)

        def normed_chunk(n):
            r = rowscale[...]
            r = jnp.concatenate([r] * (chunk // head), axis=1)
            gv = gains[l, :, pl.ds(pl.multiple_of(n * chunk, chunk), chunk)]
            return (xb[n].astype(F32) * r * gv).astype(BF16)

        def normed(g, qs):
            for q in qs:
                hb[:, (4 * g + q) * chunk:(4 * g + q + 1) * chunk] = normed_chunk(chunk_id(g, q))

        cuts = list(range(0, n_in, 512)) + [n_in]
        spans = list(zip(cuts[:-1], cuts[1:]))

        def stream_step(i, first, beside=lambda: None):
            wait(step_copies(l, i))
            beside()
            k_at = pl.ds(pl.multiple_of(i * 2 * chunk, 2 * chunk), 2 * chunk)
            rows_at = pl.ds(pl.multiple_of((i % 2) * 2 * chunk, chunk), 2 * chunk)
            for at, end in spans:
                d = jnp.dot(hb[:, k_at], wa[(i // 2) % 2, rows_at, at:end], preferred_element_type=F32)
                acc[:, at:end] = d if first else acc[:, at:end] + d

        def rest():
            normed(0, range(2, 4))
            for g in range(1, GROUPS):
                normed(g, range(4))

        if l == 0:
            normed(0, range(2))
            start(step_copies(l, 3))
            stream_step(0, True, rest)
            start(step_copies(l, 4))

            def stream(i, _):
                stream_step(i, False)
                start(step_copies(l, i + 4))
                return 0
            lax.fori_loop(1, 4, stream, 0)

            def group(g, _):
                slot = g % 2
                wait(a_copies(l, g, slot))
                k_at = pl.ds(pl.multiple_of(g * 4 * chunk, 4 * chunk), 4 * chunk)
                for at, end in spans:
                    acc[:, at:end] += jnp.dot(hb[:, k_at], wa[slot, :, at:end], preferred_element_type=F32)

                def after_two():
                    start_kv(l, 0)
                    start_kv(l, 1)
                pl.when(g == 2)(after_two)

                def after_three():
                    start(b_copies(l, 0))
                    start(b_copies(l, 1))
                pl.when(g == 3)(after_three)
                return 0
            lax.fori_loop(2, GROUPS, group, 0)
        else:
            gather_mate(0)
            normed(0, range(4))
            for n, steps in enumerate(PHASES):
                for i in steps:
                    wait(step_copies(l, i))
                for at, end in spans:
                    d = sum(jnp.dot(hb[:, i * 2 * chunk:(i + 1) * 2 * chunk],
                                    wa[i // 2 % 2, i % 2 * 2 * chunk:(i % 2 + 1) * 2 * chunk, at:end],
                                    preferred_element_type=F32) for i in steps)
                    acc[:, at:end] = d if n == 0 else acc[:, at:end] + d
                for i in steps:
                    if i + 4 < 2 * GROUPS:
                        start(step_copies(l, i + 4))
                if n + 1 < GROUPS:
                    gather_links(n + 1)
                if n > 0 and n < GROUPS:
                    gather_mate(n)
                    normed(n, range(2, 4))
                if n + 1 < GROUPS:
                    normed(n + 1, range(2))

        cosv, sinv = cosb[...], sinb[...]
        for h in range(heads):
            v = acc[:, h * head:(h + 1) * head]
            qs[h] = (v * cosv + pltpu.roll(v, head // 2, 1) * sinv).astype(BF16).astype(F32)
        v = acc[:, q_width:q_width + head]
        kr = (v * cosv + pltpu.roll(v, head // 2, 1) * sinv).astype(BF16)
        vr = acc[:, q_width + head:q_width + 2 * head].astype(BF16)
        ks[...] = kr.astype(F32)
        vs[...] = vr.astype(F32)
        kst[...] = kr
        vst[...] = vr
        start(kn_copies(l))

        gate_at = q_width + 2 * head
        for at in range(0, ff, 256):
            gv = acc[:, gate_at + at:gate_at + at + 256]
            uv = acc[:, gate_at + ff + at:gate_at + ff + at + 256]
            lhs[:, q_width + at:q_width + at + 256] = (gv * jax.nn.sigmoid(gv) * uv).astype(BF16)

        if l == 0:
            start(b_copies(l, 2))
            start(b_copies(l, 3))
        tiles = ROW_GROUP * cache_len // head
        per_tile = head // cache_len
        r_id = lax.broadcasted_iota(jnp.int32, (1, ROW_GROUP, head), 1)
        lane3 = lax.broadcasted_iota(jnp.int32, (1, ROW_GROUP, head), 2)
        tile_of = r_id // per_tile
        in_row = (lane3 // cache_len) == (r_id % per_tile)
        slot_pos = (lane3 % cache_len).astype(F32)

        def scores(at):
            keys = kb[at:at + ROW_GROUP].reshape(ROW_GROUP * cache_len, head)
            q2 = qs[:, at:at + ROW_GROUP, :].reshape(heads * ROW_GROUP, head).astype(BF16)
            s = lax.dot_general(q2, keys, (((1,), (1,)), ((), ())), preferred_element_type=F32)
            pick = s[:, 0:head].reshape(heads, ROW_GROUP, head)
            for j in range(1, tiles):
                pick = jnp.where(tile_of == j, s[:, j * head:(j + 1) * head].reshape(heads, ROW_GROUP, head), pick)
            return pick

        def weights(at, pick):
            ok = jnp.logical_and(in_row, slot_pos < lenb[at:at + ROW_GROUP, :][None])
            sc = jnp.where(ok, pick * scale, -jnp.inf)
            s_new = jnp.sum(qs[:, at:at + ROW_GROUP, :] * ks[at:at + ROW_GROUP, :][None], axis=-1, keepdims=True) * scale
            peak = jnp.maximum(jnp.max(sc, axis=-1, keepdims=True), s_new)
            w = jnp.exp(sc - peak)
            w_new = jnp.exp(s_new - peak)
            return w, w_new, jnp.sum(w, axis=-1, keepdims=True) + w_new

        def mix(at, w, w_new, den):
            vals = vb[at:at + ROW_GROUP].reshape(ROW_GROUP * cache_len, head)
            parts = [jnp.where(tile_of == j, w, 0.0).reshape(heads * ROW_GROUP, head).astype(BF16) for j in range(tiles)]
            pv = jnp.dot(jnp.concatenate(parts, axis=1), vals, preferred_element_type=F32)
            o = (pv.reshape(heads, ROW_GROUP, head) + w_new.astype(BF16).astype(F32) * vs[at:at + ROW_GROUP, :][None]) / den
            for h in range(heads):
                ob[at:at + ROW_GROUP, h * head:(h + 1) * head] = o[h]

        for p in range(KV_PIECES):
            wait(kv_copy(l, p, n) for n in range(2))
        step = STEP_ROWS
        groups_at = [list(range(b, b + step, ROW_GROUP)) for b in range(0, rows, step)]
        picks, wts = {}, {}
        for b in range(len(groups_at) + 2):
            if b < len(groups_at):
                for at in groups_at[b]:
                    picks[at] = scores(at)
            if 0 <= b - 2:
                for at in groups_at[b - 2]:
                    mix(at, *wts.pop(at))
            if 0 <= b - 1 < len(groups_at):
                for at in groups_at[b - 1]:
                    wts[at] = weights(at, picks.pop(at))
        lhs[:, 0:q_width] = ob[...].astype(BF16)

        wait(kn_copies(l))

        def drain():
            sum_drain()
            gather_drain()
            for k in range(1, members):
                stat_copy(k).wait_send()
        when(l > 0, drain)

        wait(b_copies(l, 0))
        if l == 0:
            pl.semaphore_wait(barrier, members - 1)

        def share(i):
            at = pl.multiple_of(i * blk, blk)
            return jnp.dot(lhs[...], wb[:, pl.ds(at, blk)], preferred_element_type=F32)

        send_d[0] = share(2 * opp_chip + 1 - core).astype(BF16)
        mate_top.start()
        mate_bottom.start()
        own[...] = share(2 * opp_chip + core)
        mate_top.wait_recv()
        send_o[top] = (own[top] + recv_d[0, top].astype(F32)).astype(BF16)
        opp_right.start()
        mate_bottom.wait_recv()
        send_o[bottom] = (own[bottom] + recv_d[0, bottom].astype(F32)).astype(BF16)
        opp_left.start()
        wait(b_copies(l, 1))
        wait(b_copies(l, 2))
        send_d[1] = share(2 * right_chip + 1 - core).astype(BF16)
        send_d[2] = share(2 * left_chip + 1 - core).astype(BF16)
        mate_copy(1).start()
        mate_copy(2).start()
        hold_r[...] = share(right)
        hold_l[...] = share(left)
        mate_copy(1).wait_recv()
        send_r[bottom] = (hold_r[bottom] + recv_d[1, bottom].astype(F32)).astype(BF16)
        right_bottom.start()
        mate_copy(2).wait_recv()
        send_l[top] = (hold_l[top] + recv_d[2, top].astype(F32)).astype(BF16)
        left_top.start()
        wait(b_copies(l, 3))
        if l < layers - 1:
            for i in range(4):
                start(step_copies(l + 1, i))
            start_kv(l + 1, 0)
            start_kv(l + 1, 1)
        send_d[3] = share(mate).astype(BF16)
        own[...] = share(me)
        mate_copy(3).start()
        when(l < layers - 1, lambda: start_b(l + 1))
        opp_right.wait_recv()
        send_r[top] = (hold_r[top] + recv_d[1, top].astype(F32) + opp_t[...].astype(F32)).astype(BF16)
        right_top.start()
        opp_left.wait_recv()
        send_l[bottom] = (hold_l[bottom] + recv_d[2, bottom].astype(F32) + opp_b[...].astype(F32)).astype(BF16)
        left_bottom.start()
        mate_copy(3).wait_recv()
        x_old = jnp.concatenate([xb[own_a], xb[own_b]], axis=1).astype(F32)
        own[...] = own[...] + recv_d[3].astype(F32) + x_old
        right_bottom.wait_recv()
        left_top.wait_recv()
        right_top.wait_recv()
        left_bottom.wait_recv()
        x_new = (own[...] + from_l[...].astype(F32) + from_r[...].astype(F32)).astype(BF16)
        xb[own_a] = x_new[:, :chunk]
        xb[own_b] = x_new[:, chunk:]

        def send_stats():
            v = x_new.astype(F32)
            v = v * v
            part = v[:, 0:head]
            for at in range(head, blk, head):
                part = part + v[:, at:at + head]
            col = jnp.broadcast_to(jnp.sum(part, axis=1, keepdims=True), (rows, head))
            stat_s[...] = jnp.transpose(col)[0:8]
            for k in range(1, members):
                stat_copy(k).start()
        when(l < layers - 1, send_stats)
        for c in own_sends:
            c.start()

    for l in range(layers):
        layer(l)

    out_copy(own_a).start()
    out_copy(own_b).start()
    for g in range(1, GROUPS):
        gather_links(g)
        for q in range(2):
            out_copy(chunk_id(g, q)).start()
    for g in range(GROUPS):
        gather_mate(g)
        for q in range(2, 4):
            out_copy(chunk_id(g, q)).start()
    sum_drain()
    gather_drain()
    for n in range(width // chunk):
        out_copy(n).wait()


def place(x, kn, vn, xo, ko, vo, xt, kt, vt, sem_in, sem_out):
    part = x.shape[0] // PLACE_PIECES
    loads, stores = [], []
    for n in range(PLACE_PIECES):
        r = pl.ds(n * part, part)
        loads.append(pltpu.make_async_copy(x.at[r], xt.at[r], sem_in.at[n]))
        stores.append(pltpu.make_async_copy(xt.at[r], xo.at[r], sem_out.at[n]))
    for n, (src, mid, dst) in enumerate(((kn, kt, ko), (vn, vt, vo))):
        loads.append(pltpu.make_async_copy(src, mid, sem_in.at[PLACE_PIECES + n]))
        stores.append(pltpu.make_async_copy(mid, dst, sem_out.at[PLACE_PIECES + n]))
    for c in loads:
        c.start()
    for a, b in zip(loads, stores):
        a.wait()
        b.start()
    for c in stores:
        c.wait()


def solution(mesh):
    members = mesh.shape["tp"]
    weight_col = P(None, None, "tp")
    weight_row = P(None, "tp", None)
    cache_spec = P(None, "dp", "tp", None, None)
    new_spec = P(None, "dp", "tp", None)
    row_spec = P("dp", None)
    arg_specs = (row_spec, weight_col, weight_col, weight_col, weight_row, weight_col, weight_col, weight_row,
                 P(None, None), cache_spec, cache_spec, P("dp"))

    def per_device(x_in, w_q, w_k, w_v, w_o, w_gate, w_up, w_down, norm_gain, k_cache, v_cache, lengths):
        rows, width = x_in.shape
        layers, _, q_width = w_q.shape
        cache_len, head = k_cache.shape[-2:]
        ff = w_gate.shape[-1]
        dims = (layers, rows, width, q_width, head, ff, cache_len, members)
        blk = width // members
        chunk = blk // 2
        half = rows // 2
        n_in = q_width + 2 * head + 2 * ff
        inv = np.float32(ROPE_BASE) ** (-np.arange(head // 2, dtype=np.float32) / np.float32(head // 2))
        freq = jnp.asarray(np.concatenate([inv, inv])[None].astype(np.float32))
        hbm = pl.BlockSpec(memory_space=pl.ANY)
        dma = pltpu.SemaphoreType.DMA
        x_out, k_new, v_new = pl.pallas_call(
            functools.partial(kernel, dims),
            out_shape=(jax.ShapeDtypeStruct((rows, width), BF16),
                       jax.ShapeDtypeStruct((layers, rows, head), BF16),
                       jax.ShapeDtypeStruct((layers, rows, head), BF16)),
            in_specs=[hbm] * 13,
            out_specs=(hbm, hbm, hbm),
            scratch_shapes=[
                pltpu.VMEM((width // chunk, rows, chunk), BF16),
                pltpu.VMEM((rows, n_in), F32),
                pltpu.VMEM((rows, width), BF16),
                pltpu.VMEM((2, 4 * chunk, n_in), BF16),
                pltpu.VMEM((q_width + ff, width), BF16),
                pltpu.VMEM((rows, cache_len, head), BF16),
                pltpu.VMEM((rows, cache_len, head), BF16),
                pltpu.VMEM((rows, q_width + ff), BF16),
                pltpu.VMEM((q_width // head, rows, head), F32),
                pltpu.VMEM((rows, head), F32),
                pltpu.VMEM((rows, head), F32),
                pltpu.VMEM((rows, q_width), F32),
                pltpu.VMEM((rows, head), F32),
                pltpu.VMEM((rows, head), F32),
                pltpu.VMEM((rows, head), F32),
                pltpu.VMEM((rows, head), F32),
                pltpu.VMEM((layers, 1, width), F32),
                pltpu.VMEM((rows, head), BF16),
                pltpu.VMEM((rows, head), BF16),
                pltpu.VMEM((layers, width), BF16),
                pltpu.VMEM((1, rows), jnp.int32),
                pltpu.VMEM((1, head), F32),
                pltpu.VMEM((4, rows, blk), BF16),
                pltpu.VMEM((4, rows, blk), BF16),
                pltpu.VMEM((rows, blk), BF16),
                pltpu.VMEM((rows, blk), BF16),
                pltpu.VMEM((rows, blk), BF16),
                pltpu.VMEM((half, blk), BF16),
                pltpu.VMEM((half, blk), BF16),
                pltpu.VMEM((rows, blk), BF16),
                pltpu.VMEM((rows, blk), BF16),
                pltpu.VMEM((rows, blk), F32),
                pltpu.VMEM((rows, blk), F32),
                pltpu.VMEM((rows, blk), F32),
                pltpu.VMEM((8, rows), F32),
                pltpu.VMEM((members - 1, 8, rows), F32),
                dma((2, 4, 5)), dma((2, KV_PIECES)), dma((4, 2)), dma((width // chunk,)), dma((2,)), dma((3,)),
                dma((5,)), dma((5,)), dma((2,)), dma((2,)), dma((2,)), dma((2,)), dma((2,)), dma((2,)),
                dma((6,)), dma((GROUPS, 2)), dma((2,)), dma((width // chunk,)),
                dma((members - 1,)), dma((members - 1,)),
            ],
            compiler_params=pltpu.CompilerParams(
                collective_id=0, has_side_effects=True, vmem_limit_bytes=67043328),
        )(x_in, w_q, w_k, w_v, w_o, w_gate, w_up, w_down, norm_gain, k_cache, v_cache,
          lengths.reshape(1, rows), freq)
        results = (x_out, k_new, v_new)
        x_out, k_new, v_new = pl.pallas_call(
            place,
            out_shape=tuple(jax.ShapeDtypeStruct(a.shape, a.dtype) for a in results),
            in_specs=[hbm] * 3,
            out_specs=(hbm,) * 3,
            scratch_shapes=[pltpu.VMEM(a.shape, a.dtype) for a in results]
            + [dma((PLACE_PIECES + 2,)), dma((PLACE_PIECES + 2,))],
        )(*results)
        return x_out, k_new.reshape(layers, rows, 1, head), v_new.reshape(layers, rows, 1, head)

    return jax.shard_map(per_device, mesh=mesh, in_specs=arg_specs, out_specs=(row_spec, new_spec, new_spec),
                         check_vma=False)
```
